128 devices in a mesh: seq: 16 (over z, x), grp: 8 (over y, core).
Axes of the slice: x: 4, y: 4, z: 4, core: 2. Of those that a mesh axis runs over, the one named last changes fastest.
Arguments:
- queries: bfloat16 [8, 256, 4096], P('grp', 'seq'), may hold values from -200 to 200
- prefix_keys: bfloat16 [8, 16384, 512], P('grp', 'seq'), may hold values from -20 to 20
- prefix_values: bfloat16 [8, 16384, 512], P('grp', 'seq'), may hold values from -6 to 6
- suffix_keys: bfloat16 [8, 256, 512], P('grp', 'seq'), may hold values from -48 to 48
- suffix_values: bfloat16 [8, 256, 512], P('grp', 'seq'), may hold values from -6 to 6
- parents: int32 [8, 256], P('grp'), may hold values from 0 to 255, as said below
- out_proj: bfloat16 [4096, 4096], P('seq'), may hold values from -0.09375 to 0.09375
- residual: bfloat16 [8, 256, 4096], P('grp', 'seq'), may hold values from -6 to 6
- norm_gain: float32 [4096], replicated, may hold values from 0.5 to 1.5
- router: bfloat16 [4096, 128], replicated, may hold values from -0.09375 to 0.09375
- routes: int32 [8, 256, 8], P('grp', 'seq'), may hold values from 0 to 127, all different within a row; in each aligned block of 16 rows (0 to 15, 16 to 31, ..., all dimensions but the last counted through in order) at most 2 rows name the same one
- expert_gate: bfloat16 [128, 4096, 768], P(('seq', 'grp')), may hold values from -0.09375 to 0.09375
- expert_up: bfloat16 [128, 4096, 768], P(('seq', 'grp')), may hold values from -0.09375 to 0.09375
- expert_down: bfloat16 [128, 768, 4096], P(('seq', 'grp')), may hold values from -0.21875 to 0.21875
Outputs:
- layer_out: bfloat16 [8, 256, 4096], P('grp', 'seq')
The draws below stay inside these ranges and needn't reach their ends.
Inputs may be any that keep to these rules, and one draw needn't show every extreme that they name: Each request's rows form a forest of 8 levels, each a run of 32 rows: rows of the first level are their own parents; any other row's parent is a row of the level just before its own. `routes`: among the rows of one device no expert is named more than 2 times.
All inputs are finite; a program needn't handle non-finite values.
Results may differ from the reference program's by a relative error of at most 0.012.
Values may be sent and summed in bfloat16 or wider, within the bound.
No kernel may reach another device: no remote copies, remote signals or barrier semaphores. Data moves between devices by JAX's collectives and lax.ppermute only.
A program may use at most 128 MiB of HBM per device.

```python
import math
import jax
import jax.numpy as jnp
import numpy as np
from jax import lax

D = 4096
HEADS = 32
KVH = 4
HD = 128
EFF = 768
TOP = 8
DEPTH = 8
ROWS_DEV = 16
R = 256
PREFIX = 16384
REQUESTS = 8
EXPERTS = 128
CAP = 2
N_SEQ = 16
N_GRP = 8


def prefix_base(key):
    base = jax.random.normal(jax.random.fold_in(key, 11), (REQUESTS, PREFIX, KVH * HD), jnp.float32)
    base = jnp.clip(base, -5.0, 5.0)
    position = jnp.arange(PREFIX, dtype=jnp.float32)[None, :, None] / PREFIX
    keys = base * (2.5 + position)
    return keys


def draw_prefix_keys(key, part):
    return prefix_base(key).astype(jnp.bfloat16)


def draw_queries(key, part):
    own_key = jax.random.fold_in(key, 12)
    shape = (REQUESTS, R, HEADS * HD)
    values = jnp.clip(jax.random.normal(own_key, shape, jnp.float32), -6.0, 6.0)
    return values.astype(jnp.bfloat16)


def draw_parents(key, part):
    level_size = R // DEPTH
    row = jnp.arange(R, dtype=jnp.int32)
    level = row // level_size
    offset = jax.random.randint(jax.random.fold_in(key, 21), (REQUESTS, R), 0, level_size, dtype=jnp.int32)
    parent = (level[None, :] - 1) * level_size + offset
    return jnp.where(level[None, :] == 0, row[None, :], parent).astype(jnp.int32)


def shard_levels(key, extent, cuts, least, largest):
    factor_of = 1.0
    for dim, blocks in cuts:
        heights = jax.random.uniform(jax.random.fold_in(jax.random.fold_in(key, 6), dim), (blocks,), jnp.float32, least / len(cuts), largest / len(cuts))
        factor_of = factor_of * jnp.repeat(jnp.exp(heights), extent[dim] // blocks).reshape((-1,) + (1,) * (len(extent) - 1 - dim))
    return factor_of


def deal_out(rng, own, number, rows, number_of, top, reach, slope):
    order = jax.random.permutation(rng, number_of)
    crowded, ordinary = load_shares(number_of, rows * top, reach, slope, True), load_shares(number_of, rows * top, reach, slope, False)
    places = jnp.arange(number_of)

    def named(sizes, offset_by):
        used = int((sizes > 0).sum())
        fixed = max(1, used // 4)
        moved = fixed + (places - fixed + offset_by * (used - fixed)) % max(1, number_of - fixed)
        return jnp.zeros((number_of,), jnp.int32).at[order[jnp.where(places < fixed, places, moved)]].set(jnp.asarray(sizes, jnp.int32))

    sizes = jnp.where(number % 4 == 0, named(crowded, number // 4), named(ordinary, number - number // 4 - 1))
    mixed = jax.random.permutation(jax.random.fold_in(own, 3), number_of)
    source_of, receiver = mixed[0:number_of // 2 * 2:2], mixed[1:number_of // 2 * 2:2]
    slack = jnp.minimum(sizes[source_of] - 1, reach - sizes[receiver]) // 2
    slack = jnp.where((source_of == order[0]) | (receiver == order[0]) | (sizes[receiver] == 0), 0, jnp.maximum(slack, 0))
    moved = jax.random.randint(jax.random.fold_in(own, 4), (number_of // 2,), 0, 1 << 20) % (slack + 1)
    sizes = sizes.at[source_of].add(-moved).at[receiver].add(moved)
    items = jnp.searchsorted(jnp.cumsum(sizes), jnp.arange(rows * top), side="right").astype(jnp.int32)
    table = items.reshape(top, rows).T
    table = table[jax.random.permutation(jax.random.fold_in(own, 1), rows)]
    offset_by = jax.random.randint(jax.random.fold_in(own, 2), (rows, 1), 0, top)
    return jnp.take_along_axis(table, (jnp.arange(top)[None, :] + offset_by) % top, axis=1)


def load_shares(count, total, bound, skew, full):
    loads = [(1 << 20) // math.isqrt(rank ** skew) + 1 for rank in range(1, count + 1)]
    largest = bound if full else min(bound, max(-(-total // count), total * loads[0] // sum(loads)))
    least = 1 if total - largest >= count - 1 else 0
    given, surplus = [largest] + [least] * (count - 1), total - largest - least * (count - 1)
    while surplus > 0:
        candidates = [i for i in range(1, count) if given[i] < largest] or [i for i in range(1, count) if given[i] < bound]
        mass, budget = sum([loads[i] for i in candidates]), surplus
        for i in candidates:
            addition = min(bound - given[i], max(1, budget * loads[i] // mass), surplus)
            given[i] = given[i] + addition
            surplus = surplus - addition
    return np.array(given)


def normal_values(key, extent, scale, limit, cuts=(), held_as=jnp.bfloat16):
    values = jax.random.normal(key, extent, jnp.float32) * scale
    if len(cuts) > 0:
        values = shard_levels(key, extent, cuts, -0.22, 0.18) * values
    return jnp.clip(values, min=-limit, max=limit).astype(held_as)


def setup_inputs(seed: int = 0) -> dict:
    key_of = jax.random.split(jax.random.key(seed), 15)
    queries = draw_queries(jax.random.fold_in(key_of[14], 71), 0)
    prefix_keys = draw_prefix_keys(jax.random.fold_in(key_of[14], 71), 0)
    prefix_values = normal_values(key_of[2], (REQUESTS, PREFIX, KVH * HD), 1.0, 6.0, ((0, 8), (1, 16)))
    suffix_keys = normal_values(key_of[3], (REQUESTS, R, KVH * HD), 8.0, 48.0, ((0, 8), (1, 16)))
    suffix_values = normal_values(key_of[4], (REQUESTS, R, KVH * HD), 1.0, 6.0, ((0, 8), (1, 16)))
    parents = draw_parents(jax.random.fold_in(key_of[14], 71), 0)
    out_proj = normal_values(key_of[6], (HEADS * HD, D), (HEADS * HD) ** -0.5, 0.09375, ((0, 16),))
    residual = normal_values(key_of[7], (REQUESTS, R, D), 1.0, 6.0, ((0, 8), (1, 16)))
    norm_gain = jnp.clip(1.0 + 0.1 * jax.random.normal(key_of[8], (D,), jnp.float32), 0.5, 1.5)
    router = normal_values(key_of[9], (D, EXPERTS), D ** -0.5, 0.09375)
    routes_keys = jax.random.split(jax.random.fold_in(key_of[10], 1), REQUESTS * R // ROWS_DEV)
    routes_turns = jax.random.permutation(jax.random.fold_in(key_of[10], 3), REQUESTS * R // ROWS_DEV)
    routes = jax.vmap(lambda own, number: deal_out(jax.random.fold_in(key_of[10], 2), own, number, ROWS_DEV, EXPERTS, TOP, CAP, 2))(routes_keys, routes_turns).reshape((REQUESTS, R, TOP))
    expert_gate = normal_values(key_of[11], (EXPERTS, D, EFF), D ** -0.5, 0.09375, ((0, 128),))
    expert_up = normal_values(key_of[12], (EXPERTS, D, EFF), D ** -0.5, 0.09375, ((0, 128),))
    expert_down = normal_values(key_of[13], (EXPERTS, EFF, D), EFF ** -0.5, 0.21875, ((0, 128),))
    return dict(queries=queries, prefix_keys=prefix_keys, prefix_values=prefix_values, suffix_keys=suffix_keys, suffix_values=suffix_values, parents=parents, out_proj=out_proj, residual=residual, norm_gain=norm_gain, router=router, routes=routes, expert_gate=expert_gate, expert_up=expert_up, expert_down=expert_down)


EPSILON = 1e-06

def visible_mask(parent_row):
    count = parent_row.shape[0]
    positions = jnp.arange(count, dtype=jnp.int32)
    current = positions
    visible = current[:, None] == positions[None, :]
    for level in range(DEPTH - 1):
        current = parent_row[current].astype(jnp.int32)
        visible = visible | (current[:, None] == positions[None, :])
    return visible

def request_attention(inputs):
    query_rows, key_rows, value_rows, suffix_key_rows, suffix_value_rows, parent_row = inputs
    visible = visible_mask(parent_row)
    group = HEADS // KVH
    scale = HD ** (-0.5)
    pieces = []
    for head_kv in range(KVH):
        query_block = query_rows[:, head_kv * group * HD:(head_kv + 1) * group * HD].reshape(R, group, HD).astype(jnp.float32)
        key_pre = key_rows[:, head_kv * HD:(head_kv + 1) * HD].astype(jnp.float32)
        value_pre = value_rows[:, head_kv * HD:(head_kv + 1) * HD].astype(jnp.float32)
        key_suf = suffix_key_rows[:, head_kv * HD:(head_kv + 1) * HD].astype(jnp.float32)
        value_suf = suffix_value_rows[:, head_kv * HD:(head_kv + 1) * HD].astype(jnp.float32)
        score_pre = jnp.einsum('rgd,kd->rgk', query_block, key_pre) * scale
        score_suf = jnp.einsum('rgd,jd->rgj', query_block, key_suf) * scale
        score_suf = jnp.where(visible[:, None, :], score_suf, -jnp.inf)
        top = jnp.maximum(lax.optimization_barrier(jnp.max(score_pre, axis=2)), lax.optimization_barrier(jnp.max(score_suf, axis=2)))
        weight_pre = jnp.exp(score_pre - top[:, :, None])
        weight_suf = jnp.exp(score_suf - top[:, :, None])
        total = lax.optimization_barrier(jnp.sum(weight_pre, axis=2)) + lax.optimization_barrier(jnp.sum(weight_suf, axis=2))
        rounded_pre = weight_pre.astype(jnp.bfloat16).astype(jnp.float32)
        rounded_suf = weight_suf.astype(jnp.bfloat16).astype(jnp.float32)
        summed = jnp.einsum('rgk,kd->rgd', rounded_pre, value_pre) + jnp.einsum('rgj,jd->rgd', rounded_suf, value_suf)
        pieces.append((summed / total[:, :, None]).astype(jnp.bfloat16).reshape(R, group * HD))
    return jnp.concatenate(pieces, axis=1)

def reference(queries, prefix_keys, prefix_values, suffix_keys, suffix_values, parents, out_proj, residual, norm_gain, router, routes, expert_gate, expert_up, expert_down):
    attention = lax.map(request_attention, (queries, prefix_keys, prefix_values, suffix_keys, suffix_values, parents))
    flat_attention = attention.reshape(REQUESTS * R, HEADS * HD)
    projected = jnp.dot(flat_attention, out_proj, preferred_element_type=jnp.float32)
    mixed = residual.reshape(REQUESTS * R, D).astype(jnp.float32) + projected
    inverse = lax.rsqrt(lax.optimization_barrier(jnp.mean(mixed * mixed, axis=1, keepdims=True)) + EPSILON)
    normed = (mixed * inverse * norm_gain[None, :]).astype(jnp.bfloat16)
    logits = jnp.dot(normed, router, preferred_element_type=jnp.float32)
    chosen_ids = routes.reshape(REQUESTS * R, TOP).astype(jnp.int32)
    chosen = jnp.take_along_axis(logits, chosen_ids, axis=1)
    sig = jax.nn.sigmoid(chosen)
    gates = sig / lax.optimization_barrier(jnp.sum(sig, axis=1, keepdims=True))
    flat_ids = chosen_ids.reshape(-1)
    assignments = flat_ids.shape[0]
    most_load = N_SEQ * N_GRP * CAP
    order = jnp.argsort(flat_ids, stable=True).astype(jnp.int32)
    counts = lax.optimization_barrier(jnp.sum((flat_ids[:, None] == jnp.arange(EXPERTS, dtype=jnp.int32)[None, :]).astype(jnp.int32), axis=0)).astype(jnp.int32)
    offsets = (jnp.cumsum(counts) - counts).astype(jnp.int32)
    order_padded = jnp.concatenate([order, jnp.zeros((most_load,), jnp.int32)])

    def one_expert(inputs):
        offset, count, gate_w, up_w, down_w = inputs
        index = lax.dynamic_slice(order_padded, (offset.astype(jnp.int32),), (most_load,))
        valid = jnp.arange(most_load, dtype=jnp.int32) < count
        rows = normed[index // TOP]
        gate_part = jnp.dot(rows, gate_w, preferred_element_type=jnp.float32)
        up_part = jnp.dot(rows, up_w, preferred_element_type=jnp.float32)
        act = (jax.nn.silu(gate_part) * up_part).astype(jnp.bfloat16)
        result = jnp.dot(act, down_w, preferred_element_type=jnp.float32).astype(jnp.bfloat16)
        return (index, jnp.where(valid[:, None], result, jnp.zeros_like(result)))
    indices, results = lax.map(one_expert, (offsets, counts, expert_gate, expert_up, expert_down))
    placed = jnp.zeros((assignments, D), jnp.float32).at[indices.reshape(-1)].add(results.reshape(-1, D).astype(jnp.float32))
    moe = lax.optimization_barrier(jnp.sum(placed.reshape(REQUESTS * R, TOP, D) * gates[:, :, None], axis=1))
    return (mixed + moe).astype(jnp.bfloat16).reshape(REQUESTS, R, D)
```

```python
import math

import jax
import jax.numpy as jnp
from jax import lax
from jax.experimental import pallas as pl
from jax.experimental.pallas import tpu as pltpu
from jax.sharding import PartitionSpec as P

HEADS = 32
KVH = 4
HD = 128
DEPTH = 8
EPSILON = 1e-06
GROUP = HEADS // KVH
C2 = HD ** (-0.5) * math.log2(math.e)
CAP = 2
CHUNK = 8
BF = jnp.bfloat16
F32 = jnp.float32


def params(mib=48, semantics=None):
    return pltpu.CompilerParams(
        vmem_limit_bytes=mib << 20, dimension_semantics=semantics
    )


def nt(a, b):
    return lax.dot_general(a, b, (((1,), (1,)), ((), ())), preferred_element_type=F32)


def mm(a, b):
    return jnp.dot(a, b, preferred_element_type=F32)


def hi_lo(x):
    hi = x.astype(BF)
    return hi, (x - hi.astype(F32)).astype(BF)


def attend(q, chunks):
    m = total = acc = None
    for keys, values, visible in chunks:
        s = nt(q, keys)
        if visible is not None:
            s = jnp.where(visible, s, -1e30)
        top = jnp.max(s, axis=1, keepdims=True)
        if m is not None:
            top = jnp.maximum(m, top)
        p = jnp.exp2((s - top) * C2)
        t = jnp.sum(p, axis=1, keepdims=True)
        o = mm(p.astype(BF), values)
        if m is not None:
            a = jnp.exp2((m - top) * C2)
            t = t + total * a
            o = o + acc * a
        m, total, acc = top, t, o
    return acc / total, m * C2 + jnp.log2(total)


def visible_rows(parents):
    n = parents.shape[0]
    rows = lax.broadcasted_iota(jnp.int32, (n, n), 0)
    cols = lax.broadcasted_iota(jnp.int32, (n, n), 1)
    step = ((parents == cols).astype(F32) + (rows == cols).astype(F32)).astype(BF)
    two = mm(step, step).astype(BF)
    four = mm(two, two).astype(BF)
    six = mm(four, two).astype(BF)
    return mm(six, step) > 0.5


def attention_body(own, idx, q_ref, k_ref, v_ref, b_ref, c_ref, d_ref, *rest):
    del idx
    keys = k_ref.shape[0]
    chunks = [(k_ref[...], v_ref[...], None)]
    for ref in (b_ref, c_ref, d_ref):
        chunks.append((ref[:keys, :], ref[keys:, :], None))
    if own:
        par_ref, sk_ref, sv_ref, o_ref = rest
        chunks.append((sk_ref[...], sv_ref[...], visible_rows(par_ref[...])))
    else:
        (o_ref,) = rest
    rows = q_ref.shape[0]
    lane = lax.broadcasted_iota(jnp.int32, (rows, HD), 1)
    stats = jnp.zeros((rows, HD), F32)
    for h in range(2):
        o, lse = attend(q_ref[:, h * HD : (h + 1) * HD], chunks)
        o_ref[:rows, h * HD : (h + 1) * HD] = o.astype(BF)
        left = lse
        for part in range(3):
            piece = left.astype(BF).astype(F32)
            left = left - piece
            stats = jnp.where(lane == 3 * h + part, piece, stats)
    o_ref[rows:, :] = stats.T[:16, :].astype(BF)


def attention(own, idx, q_all, keys, values, parts, extra):
    rows = q_all.shape[0]
    count = keys.shape[0]
    whole = lambda shape: pl.BlockSpec(shape, lambda i, idx: (0, 0))
    specs = [
        pl.BlockSpec((rows, 2 * HD), lambda i, idx: (0, idx[0])),
        pl.BlockSpec((count, HD), lambda i, idx: (0, idx[1])),
        pl.BlockSpec((count, HD), lambda i, idx: (0, idx[1])),
        *[whole((2 * count, HD))] * 3,
    ]
    args = [q_all, keys, values, *parts]
    if own:
        at = GROUP
        specs += [
            whole((rows, 1)),
            pl.BlockSpec((rows, HD), lambda i, idx: (0, at)),
            pl.BlockSpec((rows, HD), lambda i, idx: (0, at + 1)),
        ]
        args += [extra, q_all, q_all]
    return pl.pallas_call(
        lambda *refs: attention_body(own, *refs),
        out_shape=jax.ShapeDtypeStruct((rows + 16, 2 * HD), BF),
        grid_spec=pltpu.PrefetchScalarGridSpec(
            num_scalar_prefetch=1, grid=(1,), in_specs=specs, out_specs=whole((rows + 16, 2 * HD))
        ),
        compiler_params=params(),
        name="attend_own" if own else "attend",
    )(idx, *args)


def project_body(*refs):
    *parts, w_ref, o_ref, att = refs
    rows = att.shape[0]

    @pl.when(pl.program_id(0) == 0)
    def _():
        r = lax.broadcasted_iota(jnp.int32, (rows, rows), 0)
        c = lax.broadcasted_iota(jnp.int32, (rows, rows), 1)
        eye = (r == c).astype(F32).astype(BF)
        stats = [nt(eye, p[rows:, :]) for p in parts]
        for h in range(2):
            lse = [s[:, 3 * h : 3 * h + 1] + s[:, 3 * h + 1 : 3 * h + 2] + s[:, 3 * h + 2 : 3 * h + 3] for s in stats]
            top = jnp.maximum(jnp.maximum(lse[0], lse[1]), jnp.maximum(lse[2], lse[3]))
            w = [jnp.exp2(v - top) for v in lse]
            inv = 1.0 / (w[0] + w[1] + w[2] + w[3])
            cols = slice(h * HD, (h + 1) * HD)
            acc = sum((p[:rows, cols].astype(F32) * (v * inv) for p, v in zip(parts, w)))
            att[:, cols] = acc.astype(BF)

    o_ref[...] = mm(att[...], w_ref[...]).astype(BF)


def project(parts, weights, steps=4):
    rows, width = parts[0].shape[0] - 16, weights.shape[1]
    return pl.pallas_call(
        project_body,
        out_shape=jax.ShapeDtypeStruct((rows, width), BF),
        grid=(steps,),
        in_specs=[*[pl.BlockSpec(parts[0].shape, lambda i: (0, 0))] * 4, pl.BlockSpec((weights.shape[0], width // steps), lambda i: (0, i))],
        out_specs=pl.BlockSpec((rows, width // steps), lambda i: (0, i)),
        scratch_shapes=[pltpu.VMEM((rows, 2 * HD), BF)],
        compiler_params=params(),
        name="project",
    )(*parts, weights)


def route_body(p_ref, res_ref, gain_ref, router_ref, hot_ref, sel_ref, pack_ref, mixed_ref, gates_ref, keep):
    i = pl.program_id(0)
    rows = res_ref.shape[0]
    acc = res_ref[...].astype(F32)
    for s in range(p_ref.shape[0] // rows):
        acc = acc + p_ref[s * rows : (s + 1) * rows, :].astype(F32)
    mixed_ref[...] = acc
    keep[i] = acc

    @pl.when(i == CHUNK - 1)
    def _():
        width = CHUNK * acc.shape[1]
        square = sum(jnp.sum(keep[c] * keep[c], axis=1, keepdims=True) for c in range(CHUNK))
        inverse = lax.rsqrt(square / width + EPSILON)
        step = acc.shape[1]
        normed = [(keep[c] * inverse * gain_ref[:, c * step : (c + 1) * step]).astype(BF) for c in range(CHUNK)]
        logits = sum(mm(n, router_ref[c * step : (c + 1) * step, :]) for c, n in enumerate(normed))
        hot = hot_ref[...]
        sig = hot * jax.nn.sigmoid(logits)
        gates_ref[...] = sig / jnp.sum(sig, axis=1, keepdims=True)
        pack_ref[...] = mm(sel_ref[...], jnp.concatenate(normed, axis=0)).astype(BF)


def route(partial, residual, gain, router, hot, select):
    rows, width = residual.shape
    step = width // CHUNK
    experts = router.shape[1]
    whole = lambda shape: pl.BlockSpec(shape, lambda i: (0, 0))
    return pl.pallas_call(
        route_body,
        out_shape=(
            jax.ShapeDtypeStruct((select.shape[0], step), BF),
            jax.ShapeDtypeStruct((rows, width), F32),
            jax.ShapeDtypeStruct((rows, experts), F32),
        ),
        grid=(CHUNK,),
        in_specs=[
            pl.BlockSpec((partial.shape[0], step), lambda i: (0, i)),
            pl.BlockSpec((rows, step), lambda i: (0, i)),
            whole((1, width)),
            whole(router.shape),
            whole(hot.shape),
            whole(select.shape),
        ],
        out_specs=(
            whole((select.shape[0], step)),
            pl.BlockSpec((rows, step), lambda i: (0, i)),
            whole((rows, experts)),
        ),
        scratch_shapes=[pltpu.VMEM((CHUNK, rows, step), F32)],
        compiler_params=params(),
        name="route",
    )(partial, residual, gain, router, hot, select)


def shuffle_matrix():
    n = 16 * CAP * CHUNK
    to = lax.broadcasted_iota(jnp.int32, (n, n), 0)
    come = lax.broadcasted_iota(jnp.int32, (n, n), 1)
    tokens = 16 * CAP
    chunk = come % CHUNK
    token = come // CHUNK
    return (to == chunk * tokens + token).astype(F32).astype(BF)


def expert_body(x_ref, perm_ref, back_ref, g_ref, u_ref, d_ref, o_ref, x, gate, up, act, y):
    i = pl.program_id(0)
    block = perm_ref.shape[0]
    tokens = block // CHUNK
    step = x_ref.shape[1]

    @pl.when(i == 0)
    def _():
        for b in range(x_ref.shape[0] // block):
            z = mm(perm_ref[...], x_ref[b * block : (b + 1) * block, :]).astype(BF)
            for c in range(CHUNK):
                x[c, b * tokens : (b + 1) * tokens, :] = z[c * tokens : (c + 1) * tokens, :]
        gate[...] = jnp.zeros_like(gate)
        up[...] = jnp.zeros_like(up)

    @pl.when(i < CHUNK)
    def _():
        piece = x[jnp.minimum(i, CHUNK - 1)]
        gate[...] += mm(piece, g_ref[...])
        up[...] += mm(piece, u_ref[...])

    @pl.when(i == CHUNK - 1)
    def _():
        act[...] = (jax.nn.silu(gate[...]) * up[...]).astype(BF)

    @pl.when(i >= CHUNK)
    def _():
        y[jnp.maximum(i - CHUNK, 0)] = mm(act[...], d_ref[...]).astype(BF)

    @pl.when(i == 2 * CHUNK - 1)
    def _():
        for b in range(o_ref.shape[0] // block):
            z = jnp.concatenate([y[c, b * tokens : (b + 1) * tokens, :] for c in range(CHUNK)], axis=0)
            o_ref[b * block : (b + 1) * block, :] = mm(back_ref[...], z).astype(BF)


def expert(arrived, perm, back, gate_w, up_w, down_w):
    width, hidden = gate_w.shape
    step = width // CHUNK
    total = arrived.shape[0]
    tokens = total // CHUNK
    whole = lambda shape: pl.BlockSpec(shape, lambda i: (0, 0))
    first = lambda i: (jnp.minimum(i, CHUNK - 1), 0)
    return pl.pallas_call(
        expert_body,
        out_shape=jax.ShapeDtypeStruct(arrived.shape, BF),
        grid=(2 * CHUNK,),
        in_specs=[
            whole(arrived.shape),
            whole(perm.shape),
            whole(back.shape),
            pl.BlockSpec((step, hidden), first),
            pl.BlockSpec((step, hidden), first),
            pl.BlockSpec((hidden, step), lambda i: (0, jnp.maximum(i - CHUNK, 0))),
        ],
        out_specs=whole(arrived.shape),
        scratch_shapes=[
            pltpu.VMEM((CHUNK, tokens, step), BF),
            pltpu.VMEM((tokens, hidden), F32),
            pltpu.VMEM((tokens, hidden), F32),
            pltpu.VMEM((tokens, hidden), BF),
            pltpu.VMEM((CHUNK, tokens, step), BF),
        ],
        compiler_params=params(),
        name="expert",
    )(arrived, perm, back, gate_w, up_w, down_w)


def finish_body(ret_ref, mask_ref, gates_ref, mixed_ref, o_ref):
    rows, experts = gates_ref.shape
    span = ret_ref.shape[0]
    step = ret_ref.shape[1]
    e = lax.broadcasted_iota(jnp.int32, (experts, span), 0)
    at = lax.broadcasted_iota(jnp.int32, (experts, span), 1)
    spread = (e == at // (span // experts)).astype(F32).astype(BF)
    high, low = hi_lo(gates_ref[...])
    wide = mm(high, spread) + mm(low, spread)
    weights = jnp.concatenate([wide] * CHUNK, axis=0) * mask_ref[...].astype(F32)
    high, low = hi_lo(weights)
    moe = mm(high, ret_ref[...]) + mm(low, ret_ref[...])
    for c in range(CHUNK):
        cols = slice(c * step, (c + 1) * step)
        o_ref[:, cols] = (mixed_ref[:, cols] + moe[c * rows : (c + 1) * rows, :]).astype(BF)


def finish(returned, mask, gates, mixed):
    return pl.pallas_call(
        finish_body,
        out_shape=jax.ShapeDtypeStruct(mixed.shape, BF),
        compiler_params=params(),
        name="finish",
    )(returned, mask, gates, mixed)


def local(
    queries,
    prefix_keys,
    prefix_values,
    suffix_keys,
    suffix_values,
    parents,
    out_proj,
    residual,
    norm_gain,
    router,
    routes,
    expert_gate,
    expert_up,
    expert_down,
):
    seq_count = lax.axis_size("seq")
    side = KVH
    across = seq_count // side
    s = lax.axis_index("seq")
    z, x = s // across, s % across
    q, sk, sv = queries[0], suffix_keys[0], suffix_values[0]
    rows = q.shape[0]
    keys, values = prefix_keys[0], prefix_values[0]
    cut = lambda a: jnp.moveaxis(a.reshape(rows, side, -1), 1, 0)
    both = jnp.concatenate([cut(q), cut(sk), cut(sv)], axis=2)
    copies = jnp.broadcast_to(both[:, None], (side, across, *both.shape[1:])).reshape(seq_count, rows, -1)
    parts = []
    for d in (1, 3, 2):
        head = (z + d) % side
        piece = jnp.concatenate(
            [lax.dynamic_slice_in_dim(a, head * HD, HD, 1) for a in (keys, values)], axis=0
        )
        parts.append(lax.ppermute(piece, "seq", [(i, (i + d * across) % seq_count) for i in range(seq_count)]))
    q_all = lax.all_to_all(copies, "seq", 0, 0, tiled=True).reshape(seq_count * rows, -1)
    blocks = []
    for d in (1, 3, 2, 0):
        idx = jnp.stack([(x + d) % across, z]).astype(jnp.int32)
        block = attention(d == 0, idx, q_all, keys, values, parts, parents[0][:, None])
        if d:
            perm = [(i, i // across * across + (i + d) % across) for i in range(seq_count)]
            block = lax.ppermute(block, "seq", perm)
        blocks.append(block)
    projected = project(blocks, out_proj)
    arrived = lax.all_to_all(
        projected.reshape(seq_count, rows, -1), "seq", 0, 0, tiled=True
    ).reshape(projected.shape)
    experts = router.shape[1]
    ids = routes[0]
    hot = jnp.any(ids[:, :, None] == jnp.arange(experts, dtype=jnp.int32), axis=1)
    before = jnp.cumsum(hot.astype(jnp.int32), axis=0) - hot
    slots = hot[:, :, None] & (before[:, :, None] == jnp.arange(CAP, dtype=jnp.int32))
    same = jnp.eye(CHUNK, dtype=jnp.bool_)
    mask = slots[None, :, :, :, None] & same[:, None, None, None, :]
    mask = mask.reshape(CHUNK * rows, experts * CAP * CHUNK).astype(BF)
    chosen = jnp.moveaxis(slots, 0, 2)
    select = chosen[:, :, None, None, :] & same[None, None, :, :, None]
    select = select.reshape(experts * CAP * CHUNK, CHUNK * rows).astype(BF)
    packed, mixed, gates = route(arrived, residual[0], norm_gain[None, :], router, hot.astype(F32), select)
    exchange = lambda a: lax.all_to_all(
        a.reshape(experts, CAP * CHUNK, -1), ("seq", "grp"), 0, 0, tiled=True
    ).reshape(a.shape)
    order = shuffle_matrix()
    finished = expert(exchange(packed), order, order.T, expert_gate[0], expert_up[0], expert_down[0])
    return finish(exchange(finished), mask, gates, mixed)[None]


def solution(mesh):
    rows = P("grp", "seq", None)
    spread = P(("seq", "grp"), None, None)
    in_specs = (
        rows, rows, rows, rows, rows, P("grp", None), P("seq", None), rows, P(), P(), rows, spread, spread, spread,
    )
    return jax.shard_map(local, mesh=mesh, in_specs=in_specs, out_specs=rows, check_vma=False)
```

```python
import math

import jax
import jax.numpy as jnp
from jax import lax
from jax.experimental import pallas as pl
from jax.experimental.pallas import tpu as pltpu
from jax.sharding import PartitionSpec as P

HEADS = 32
KVH = 4
HD = 128
DEPTH = 8
EPSILON = 1e-06
GROUP = HEADS // KVH
C2 = HD ** (-0.5) * math.log2(math.e)
CAP = 2
CHUNK = 8
BF = jnp.bfloat16
F32 = jnp.float32


def params(mib=48, semantics=None):
    return pltpu.CompilerParams(
        vmem_limit_bytes=mib << 20, dimension_semantics=semantics
    )


def nt(a, b):
    return lax.dot_general(a, b, (((1,), (1,)), ((), ())), preferred_element_type=F32)


def mm(a, b):
    return jnp.dot(a, b, preferred_element_type=F32)


def hi_lo(x):
    hi = x.astype(BF)
    return hi, (x - hi.astype(F32)).astype(BF)


def scores(q, chunks, s_ref):
    top, at = None, 0
    for k, visible in chunks:
        s = nt(q, k) * C2
        if visible is not None:
            s = jnp.where(visible, s, -1e30)
        s_ref[:, at : at + k.shape[0]] = s
        m = jnp.max(s, axis=1, keepdims=True)
        top = m if top is None else jnp.maximum(top, m)
        at += k.shape[0]
    return top


def weigh(s_ref, values, top, state, span=512):
    if state is not None:
        before, lse = state
        top = jnp.maximum(top, lse)
    acc = None
    for at in range(0, s_ref.shape[1], span):
        cols = slice(at, min(at + span, s_ref.shape[1]))
        part = mm(jnp.exp2(s_ref[:, cols] - top).astype(BF), values[cols, :])
        acc = part if acc is None else acc + part
    out, total = acc[:, :HD], acc[:, HD : HD + 1]
    if state is not None:
        a = jnp.exp2(lse - top)
        out, total = out + before * a, total + a
    return out / total, top + jnp.log2(total)


def with_ones(ref, values):
    at = 0
    for v in values:
        ref[at : at + v.shape[0], :HD] = v
        ref[at : at + v.shape[0], HD:] = jnp.ones(v.shape, BF)
        at += v.shape[0]


def lane_of(stats, h):
    lane = lax.broadcasted_iota(jnp.int32, stats.shape, 1)
    return jnp.sum(jnp.where(lane == h, stats, 0.0), axis=1, keepdims=True)


def visible_rows(parents):
    n = parents.shape[0]
    rows = lax.broadcasted_iota(jnp.int32, (n, n), 0)
    cols = lax.broadcasted_iota(jnp.int32, (n, n), 1)
    step = ((parents == cols).astype(F32) + (rows == cols).astype(F32)).astype(BF)
    two = mm(step, step).astype(BF)
    four = mm(two, two).astype(BF)
    six = mm(four, two).astype(BF)
    return mm(six, step) > 0.5


def heads_body(k_refs, v_refs, q_ref, before, o_ref, l_ref, v1, s0, s1):
    chunks = [(r[...], None) for r in k_refs]
    with_ones(v1, [r[...] for r in v_refs])

    def q_of(h):
        return q_ref[:, pl.ds(pl.multiple_of(h * HD, HD), HD)]

    def one(h, s_ref, top, stats):
        cols = pl.ds(pl.multiple_of(h * HD, HD), HD)
        state = None if before is None else (before[0][:, cols], lane_of(before[1][...], h))
        o, lse = weigh(s_ref, v1, top, state)
        o_ref[:, cols] = o
        lane = lax.broadcasted_iota(jnp.int32, stats.shape, 1)
        return jnp.where(lane == h, lse, stats)

    def pair(i, carry):
        top, stats = carry
        h = 2 * i
        after = scores(q_of(h + 1), chunks, s1)
        stats = one(h, s0, top, stats)
        top = scores(q_of(jnp.minimum(h + 2, GROUP - 1)), chunks, s0)
        return top, one(h + 1, s1, after, stats)

    first = scores(q_of(0), chunks, s0)
    l_ref[...] = lax.fori_loop(0, GROUP // 2, pair, (first, jnp.zeros(l_ref.shape, F32)))[1]


def state_shapes(rows):
    return [jax.ShapeDtypeStruct((rows, GROUP * HD), F32), jax.ShapeDtypeStruct((rows, HD), F32)]


def heads_scratch(rows, count):
    return [pltpu.VMEM((count, 2 * HD), BF), pltpu.VMEM((rows, count), F32), pltpu.VMEM((rows, count), F32)]


def start_body(idx, q_ref, k_ref, v_ref, o_ref, l_ref, *scratch):
    del idx
    heads_body([k_ref], [v_ref], q_ref, None, o_ref, l_ref, *scratch)


def attend_start(idx, q_all, keys, values):
    rows, count = q_all.shape[0], keys.shape[0]
    whole = lambda shape: pl.BlockSpec(shape, lambda i, idx: (0, 0))
    return pl.pallas_call(
        start_body,
        out_shape=state_shapes(rows),
        grid_spec=pltpu.PrefetchScalarGridSpec(
            num_scalar_prefetch=1,
            grid=(1,),
            in_specs=[
                whole(q_all.shape),
                pl.BlockSpec((count, HD), lambda i, idx: (0, idx[1])),
                pl.BlockSpec((count, HD), lambda i, idx: (0, idx[1])),
            ],
            out_specs=[whole(v.shape) for v in state_shapes(rows)],
            scratch_shapes=heads_scratch(rows, count),
        ),
        compiler_params=params(24),
        name="attend_start",
    )(idx, q_all, keys, values)


def more_body(q_ref, so_ref, sl_ref, b_ref, c_ref, o_ref, l_ref, *scratch):
    n = b_ref.shape[0] // 2
    keys, values = [[r.at[at] for r in (b_ref, c_ref)] for at in (pl.ds(0, n), pl.ds(n, n))]
    heads_body(keys, values, q_ref, (so_ref, sl_ref), o_ref, l_ref, *scratch)


def attend_more(q_all, state, parts):
    rows = q_all.shape[0]
    return pl.pallas_call(
        more_body,
        out_shape=state_shapes(rows),
        scratch_shapes=heads_scratch(rows, parts[0].shape[0]),
        compiler_params=params(24),
        name="attend_more",
    )(q_all, *state, *parts)


def last_body(own, idx, q_ref, so_ref, sl_ref, b_ref, *rest):
    n = b_ref.shape[0] // 2
    chunks, values = [(b_ref[:n, :], None)], [b_ref[n:, :]]
    if own:
        par_ref, sk_ref, sv_ref, o_ref, v1, s0, s1 = rest
        chunks.append((sk_ref[...], visible_rows(par_ref[...])))
        values.append(sv_ref[...])
    else:
        o_ref, v1, s0, s1 = rest
    with_ones(v1, values)
    rows = q_ref.shape[0]
    lane = lax.broadcasted_iota(jnp.int32, (rows, HD), 1)
    stats = jnp.zeros((rows, HD), F32)
    tops = [scores(q_ref[:, h * HD : (h + 1) * HD], chunks, s) for h, s in enumerate((s0, s1))]
    for h, s in enumerate((s0, s1)):
        cols = slice(h * HD, (h + 1) * HD)
        state = so_ref[:, cols], lane_of(sl_ref[...], 2 * idx[0] + h)
        o, lse = weigh(s, v1, tops[h], state)
        o_ref[:rows, cols] = o.astype(BF)
        left = lse
        for part in range(3):
            piece = left.astype(BF).astype(F32)
            left = left - piece
            stats = jnp.where(lane == 3 * h + part, piece, stats)
    o_ref[rows:, :] = stats.T[:16, :].astype(BF)


def attend_last(own, idx, q_all, state, part, extra):
    rows = q_all.shape[0]
    whole = lambda shape: pl.BlockSpec(shape, lambda i, idx: (0, 0))
    pair = pl.BlockSpec((rows, 2 * HD), lambda i, idx: (0, idx[0]))
    specs = [pair, pair, whole((rows, HD)), whole(part.shape)]
    args = [q_all, *state, part]
    count = part.shape[0] // 2
    if own:
        at = GROUP
        specs += [
            whole((rows, 1)),
            pl.BlockSpec((rows, HD), lambda i, idx: (0, at)),
            pl.BlockSpec((rows, HD), lambda i, idx: (0, at + 1)),
        ]
        args += [extra, q_all, q_all]
        count += rows
    return pl.pallas_call(
        lambda *refs: last_body(own, *refs),
        out_shape=jax.ShapeDtypeStruct((rows + 16, 2 * HD), BF),
        grid_spec=pltpu.PrefetchScalarGridSpec(
            num_scalar_prefetch=1,
            grid=(1,),
            in_specs=specs,
            out_specs=whole((rows + 16, 2 * HD)),
            scratch_shapes=heads_scratch(rows, count),
        ),
        compiler_params=params(24),
        name="attend_own" if own else "attend_last",
    )(idx, *args)


def combine(parts, att):
    rows = att.shape[0]
    r = lax.broadcasted_iota(jnp.int32, (rows, rows), 0)
    c = lax.broadcasted_iota(jnp.int32, (rows, rows), 1)
    eye = (r == c).astype(F32).astype(BF)
    stats = [nt(eye, p[rows:, :]) for p in parts]
    for h in range(2):
        at = 3 * h
        lse = [s[:, at : at + 1] + s[:, at + 1 : at + 2] + s[:, at + 2 : at + 3] for s in stats]
        top = jnp.maximum(jnp.maximum(lse[0], lse[1]), jnp.maximum(lse[2], lse[3]))
        w = [jnp.exp2(v - top) for v in lse]
        inv = 1.0 / (w[0] + w[1] + w[2] + w[3])
        cols = slice(h * HD, (h + 1) * HD)
        acc = sum(p[:rows, cols].astype(F32) * (v * inv) for p, v in zip(parts, w))
        att[:, cols] = acc.astype(BF)


def project_body(*refs):
    *parts, w_ref, o_ref, att = refs

    @pl.when(pl.program_id(0) == 0)
    def _():
        combine(parts, att)

    o_ref[...] = mm(att[...], w_ref[...]).astype(BF)


def project(parts, weights, steps=4):
    rows, width = parts[0].shape[0] - 16, weights.shape[1]
    return pl.pallas_call(
        project_body,
        out_shape=pltpu.HBM((rows, width), BF),
        grid=(steps,),
        in_specs=[
            *[pl.BlockSpec(parts[0].shape, lambda i: (0, 0))] * 4,
            pl.BlockSpec((weights.shape[0], width // steps), lambda i: (0, i)),
        ],
        out_specs=pl.BlockSpec((rows, width // steps), lambda i: (0, i)),
        scratch_shapes=[pltpu.VMEM((rows, 2 * HD), BF)],
        compiler_params=params(24),
        name="project",
    )(*parts, weights)


def route_body(p_ref, res_ref, gain_ref, router_ref, hot_ref, sel_ref, pack_ref, mixed_ref, gates_ref, buf, sem):
    rows, width = res_ref.shape
    step = width // CHUNK
    kept = []
    for c in range(CHUNK):
        cols = slice(c * step, (c + 1) * step)
        acc = res_ref[:, cols].astype(F32)
        for j in range(p_ref.shape[0] // rows):
            acc = acc + p_ref[j * rows : (j + 1) * rows, cols].astype(F32)
        mixed_ref[:, cols] = acc
        kept.append(acc)
    square = sum(jnp.sum(a * a, axis=1, keepdims=True) for a in kept)
    inverse = lax.rsqrt(square / width + EPSILON)
    normed = [(a * inverse * gain_ref[:, c * step : (c + 1) * step]).astype(BF) for c, a in enumerate(kept)]
    rows = jnp.concatenate(normed, axis=0)
    pieces = pack_ref.shape[0] // 4
    copies = []
    for j in range(4):
        at = pl.ds(j * pieces, pieces)
        buf[at, :] = mm(sel_ref[at, :], rows).astype(BF)
        copies.append(pltpu.make_async_copy(buf.at[at], pack_ref.at[at], sem.at[j]))
        copies[-1].start()
    logits = sum(mm(n, router_ref[c * step : (c + 1) * step, :]) for c, n in enumerate(normed))
    sig = hot_ref[...] * jax.nn.sigmoid(logits)
    gates_ref[...] = sig / jnp.sum(sig, axis=1, keepdims=True)
    for copy in copies:
        copy.wait()


def route(partial, residual, gain, router, hot, select):
    rows, width = residual.shape
    step = width // CHUNK
    experts = router.shape[1]
    whole = lambda shape: pl.BlockSpec(shape, lambda i: (0, 0))
    args = (partial, residual, gain, router, hot, select)
    return pl.pallas_call(
        route_body,
        out_shape=(
            pltpu.HBM((select.shape[0], step), BF),
            jax.ShapeDtypeStruct((rows, width), F32),
            jax.ShapeDtypeStruct((rows, experts), F32),
        ),
        grid=(1,),
        in_specs=[whole(v.shape) for v in args],
        out_specs=(
            pl.BlockSpec(memory_space=pltpu.HBM),
            whole((rows, width)),
            whole((rows, experts)),
        ),
        scratch_shapes=[pltpu.VMEM((select.shape[0], step), BF), pltpu.SemaphoreType.DMA((4,))],
        compiler_params=params(),
        name="route",
    )(*args)


def shuffle_matrix():
    n = 16 * CAP * CHUNK
    to = lax.broadcasted_iota(jnp.int32, (n, n), 0)
    come = lax.broadcasted_iota(jnp.int32, (n, n), 1)
    tokens = 16 * CAP
    chunk = come % CHUNK
    token = come // CHUNK
    return (to == chunk * tokens + token).astype(F32).astype(BF)


STEPS = 4


def expert_body(perm_ref, back_ref, x_in, g_hbm, u_hbm, d_hbm, o_hbm, x, g, u, d, act, y, out, sems, out_sems):
    block = perm_ref.shape[0]
    tokens = block // CHUNK
    depth = g.shape[1]
    span = d.shape[2]
    count = x_in.shape[0] // block
    fetch = []
    for k in range(STEPS):
        for j, (src, dst) in enumerate(((g_hbm, g), (u_hbm, u))):
            at = pl.ds(k * depth, depth)
            fetch.append(pltpu.make_async_copy(src.at[at, :], dst.at[k], sems.at[2 * k + j]))
    for k in range(STEPS):
        at = pl.ds(k * span, span)
        fetch.append(pltpu.make_async_copy(d_hbm.at[:, at], d.at[k], sems.at[2 * STEPS + k]))
    for copy in fetch:
        copy.start()
    step = x_in.shape[1]
    for b in range(count):
        z = mm(perm_ref[...], x_in[b * block : (b + 1) * block, :]).astype(BF)
        for c in range(CHUNK):
            x[b * tokens : (b + 1) * tokens, c * step : (c + 1) * step] = z[c * tokens : (c + 1) * tokens, :]
    gate = up = None
    for k in range(STEPS):
        piece = x[:, k * depth : (k + 1) * depth]
        fetch[2 * k].wait()
        part = mm(piece, g[k])
        gate = part if gate is None else gate + part
        fetch[2 * k + 1].wait()
        part = mm(piece, u[k])
        up = part if up is None else up + part
    act[...] = (jax.nn.silu(gate) * up).astype(BF)
    for k in range(STEPS):
        fetch[2 * STEPS + k].wait()
        y[:, k * span : (k + 1) * span] = mm(act[...], d[k]).astype(BF)
    sends = []
    for b in range(count):
        rows = slice(b * tokens, (b + 1) * tokens)
        z = jnp.concatenate([y[rows, c * step : (c + 1) * step] for c in range(CHUNK)], axis=0)
        at = pl.ds(b * block, block)
        out[at, :] = mm(back_ref[...], z).astype(BF)
        sends.append(pltpu.make_async_copy(out.at[at], o_hbm.at[at], out_sems.at[b]))
        sends[-1].start()
    for copy in sends:
        copy.wait()


def expert(arrived, perm, back, gate_w, up_w, down_w):
    width, hidden = gate_w.shape
    total, step = arrived.shape
    tokens = total // CHUNK
    blocks = total // perm.shape[0]
    whole = lambda shape: pl.BlockSpec(shape, lambda i: (0, 0))
    hbm = pl.BlockSpec(memory_space=pltpu.HBM)
    return pl.pallas_call(
        expert_body,
        out_shape=pltpu.HBM(arrived.shape, BF),
        grid=(1,),
        in_specs=[whole(perm.shape), whole(back.shape), whole(arrived.shape), hbm, hbm, hbm],
        out_specs=hbm,
        scratch_shapes=[
            pltpu.VMEM((tokens, width), BF),
            pltpu.VMEM((STEPS, width // STEPS, hidden), BF),
            pltpu.VMEM((STEPS, width // STEPS, hidden), BF),
            pltpu.VMEM((STEPS, hidden, width // STEPS), BF),
            pltpu.VMEM((tokens, hidden), BF),
            pltpu.VMEM((tokens, width), BF),
            pltpu.VMEM((total, step), BF),
            pltpu.SemaphoreType.DMA((3 * STEPS,)),
            pltpu.SemaphoreType.DMA((blocks,)),
        ],
        compiler_params=params(),
        name="expert",
    )(perm, back, arrived, gate_w, up_w, down_w)


def finish_body(ret_ref, mask_ref, gates_ref, mixed_ref, o_ref):
    rows, experts = gates_ref.shape
    span = ret_ref.shape[0]
    step = ret_ref.shape[1]
    e = lax.broadcasted_iota(jnp.int32, (experts, span), 0)
    at = lax.broadcasted_iota(jnp.int32, (experts, span), 1)
    spread = (e == at // (span // experts)).astype(F32).astype(BF)
    high, low = hi_lo(gates_ref[...])
    wide = mm(high, spread) + mm(low, spread)
    weights = jnp.concatenate([wide] * CHUNK, axis=0) * mask_ref[...].astype(F32)
    high, low = hi_lo(weights)
    moe = mm(high, ret_ref[...]) + mm(low, ret_ref[...])
    for c in range(CHUNK):
        cols = slice(c * step, (c + 1) * step)
        o_ref[:, cols] = (mixed_ref[:, cols] + moe[c * rows : (c + 1) * rows, :]).astype(BF)


def finish(returned, mask, gates, mixed):
    return pl.pallas_call(
        finish_body,
        out_shape=jax.ShapeDtypeStruct(mixed.shape, BF),
        compiler_params=params(),
        name="finish",
    )(returned, mask, gates, mixed)


def ready_body(q_ref, k_ref, v_ref, o_ref):
    rows, side = q_ref.shape[0], KVH
    across = o_ref.shape[0] // rows // side
    wide = q_ref.shape[1] // side
    for z in range(side):
        for x in range(across):
            at = slice((z * across + x) * rows, (z * across + x + 1) * rows)
            o_ref[at, :wide] = q_ref[:, z * wide : (z + 1) * wide]
            o_ref[at, wide : wide + HD] = k_ref[:, z * HD : (z + 1) * HD]
            o_ref[at, wide + HD :] = v_ref[:, z * HD : (z + 1) * HD]


def ready(q, k, v, devices):
    rows = q.shape[0]
    return pl.pallas_call(
        ready_body,
        out_shape=pltpu.HBM((devices * rows, (GROUP + 2) * HD), BF),
        compiler_params=params(24),
        name="ready",
    )(q, k, v)


def local(
    queries,
    prefix_keys,
    prefix_values,
    suffix_keys,
    suffix_values,
    parents,
    out_proj,
    residual,
    norm_gain,
    router,
    routes,
    expert_gate,
    expert_up,
    expert_down,
):
    seq_count = lax.axis_size("seq")
    side = KVH
    across = seq_count // side
    s = lax.axis_index("seq")
    z, x = s // across, s % across
    q, sk, sv = queries[0], suffix_keys[0], suffix_values[0]
    rows = q.shape[0]
    keys, values = prefix_keys[0], prefix_values[0]
    copies = ready(q, sk, sv, seq_count)
    parts = []
    for d in (1, 3, 2):
        head = (z + d) % side
        piece = jnp.concatenate(
            [lax.dynamic_slice_in_dim(a, head * HD, HD, 1) for a in (keys, values)], axis=0
        )
        parts.append(lax.ppermute(piece, "seq", [(i, (i + d * across) % seq_count) for i in range(seq_count)]))
    q_all = lax.all_to_all(copies.reshape(seq_count, rows, -1), "seq", 0, 0, tiled=True).reshape(copies.shape)
    place = jnp.stack([x, z]).astype(jnp.int32)
    state = attend_start(place, q_all, keys, values)
    state = attend_more(q_all, state, parts[:2])
    along_x = lambda a, d: lax.ppermute(
        a, "seq", [(i, i // across * across + (i + d) % across) for i in range(seq_count)]
    )
    blocks = []
    for d in (2, 1, 3, 0):
        idx = jnp.stack([(x + d) % across, z]).astype(jnp.int32)
        block = attend_last(d == 0, idx, q_all, state, parts[2], parents[0][:, None])
        blocks.append(along_x(block, d) if d else block)
    projected = project(blocks, out_proj)
    arrived = lax.all_to_all(
        projected.reshape(seq_count, rows, -1), "seq", 0, 0, tiled=True
    ).reshape(projected.shape)
    experts = router.shape[1]
    ids = routes[0]
    hot = jnp.any(ids[:, :, None] == jnp.arange(experts, dtype=jnp.int32), axis=1)
    before = jnp.cumsum(hot.astype(jnp.int32), axis=0) - hot
    slots = hot[:, :, None] & (before[:, :, None] == jnp.arange(CAP, dtype=jnp.int32))
    same = jnp.eye(CHUNK, dtype=jnp.bool_)
    mask = slots[None, :, :, :, None] & same[:, None, None, None, :]
    mask = mask.reshape(CHUNK * rows, experts * CAP * CHUNK).astype(BF)
    chosen = jnp.moveaxis(slots, 0, 2)
    select = chosen[:, :, None, None, :] & same[None, None, :, :, None]
    select = select.reshape(experts * CAP * CHUNK, CHUNK * rows).astype(BF)
    packed, mixed, gates = route(arrived, residual[0], norm_gain[None, :], router, hot.astype(F32), select)
    exchange = lambda a: lax.all_to_all(
        a.reshape(experts, CAP * CHUNK, -1), ("seq", "grp"), 0, 0, tiled=True
    ).reshape(a.shape)
    order = shuffle_matrix()
    finished = expert(exchange(packed), order, order.T, expert_gate[0], expert_up[0], expert_down[0])
    return finish(exchange(finished), mask, gates, mixed)[None]


def solution(mesh):
    rows = P("grp", "seq", None)
    spread = P(("seq", "grp"), None, None)
    in_specs = (
        rows, rows, rows, rows, rows, P("grp", None), P("seq", None), rows, P(), P(), rows, spread, spread, spread,
    )
    return jax.shard_map(local, mesh=mesh, in_specs=in_specs, out_specs=rows, check_vma=False)
```

```python
import math

import jax
import jax.numpy as jnp
from jax import lax
from jax.experimental import pallas as pl
from jax.experimental.pallas import tpu as pltpu
from jax.sharding import PartitionSpec as P


HEADS = 32
KVH = 4
HD = 128
EPSILON = 1e-06
GROUP = HEADS // KVH
C2 = HD ** (-0.5) * math.log2(math.e)
CAP = 2
CHUNK = 8
BF = jnp.bfloat16
F32 = jnp.float32


def params(mib=48, semantics=None):
    return pltpu.CompilerParams(
        vmem_limit_bytes=mib << 20, dimension_semantics=semantics
    )


def nt(a, b):
    return lax.dot_general(a, b, (((1,), (1,)), ((), ())), preferred_element_type=F32)


def mm(a, b):
    return jnp.dot(a, b, preferred_element_type=F32)


def hi_lo(x):
    hi = x.astype(BF)
    return hi, (x - hi.astype(F32)).astype(BF)


def scores(q, chunks, s_ref):
    top, at = None, 0
    for k, visible in chunks:
        s = nt(q, k) * C2
        if visible is not None:
            s = jnp.where(visible, s, -1e30)
        s_ref[:, at : at + k.shape[0]] = s
        m = jnp.max(s, axis=1, keepdims=True)
        top = m if top is None else jnp.maximum(top, m)
        at += k.shape[0]
    return top


def weigh(s_ref, values, top, state, span=512):
    if state is not None:
        before, lse = state
        top = jnp.maximum(top, lse)
    acc = None
    for at in range(0, s_ref.shape[1], span):
        cols = slice(at, min(at + span, s_ref.shape[1]))
        part = mm(jnp.exp2(s_ref[:, cols] - top).astype(BF), values[cols, :])
        acc = part if acc is None else acc + part
    out, total = acc[:, :HD], acc[:, HD : HD + 1]
    if state is not None:
        a = jnp.exp2(lse - top)
        out, total = out + before * a, total + a
    return out / total, top + jnp.log2(total)


def with_ones(ref, values):
    at = 0
    for v in values:
        ref[at : at + v.shape[0], :HD] = v
        ref[at : at + v.shape[0], HD:] = jnp.ones(v.shape, BF)
        at += v.shape[0]


def lane_of(stats, h):
    lane = lax.broadcasted_iota(jnp.int32, stats.shape, 1)
    return jnp.sum(jnp.where(lane == h, stats, 0.0), axis=1, keepdims=True)


def visible_rows(parents):
    n = parents.shape[0]
    rows = lax.broadcasted_iota(jnp.int32, (n, n), 0)
    cols = lax.broadcasted_iota(jnp.int32, (n, n), 1)
    step = ((parents == cols).astype(F32) + (rows == cols).astype(F32)).astype(BF)
    two = mm(step, step).astype(BF)
    four = mm(two, two).astype(BF)
    six = mm(four, two).astype(BF)
    return mm(six, step) > 0.5


def heads_body(k_refs, v_refs, q_ref, before, o_ref, l_ref, v1, s0, s1):
    chunks = [(r[...], None) for r in k_refs]
    with_ones(v1, [r[...] for r in v_refs])

    def q_of(h):
        return q_ref[:, pl.ds(pl.multiple_of(h * HD, HD), HD)]

    def one(h, s_ref, top, stats):
        cols = pl.ds(pl.multiple_of(h * HD, HD), HD)
        state = None if before is None else (before[0][:, cols], lane_of(before[1][...], h))
        o, lse = weigh(s_ref, v1, top, state)
        o_ref[:, cols] = o
        lane = lax.broadcasted_iota(jnp.int32, stats.shape, 1)
        return jnp.where(lane == h, lse, stats)

    def pair(i, carry):
        top, stats = carry
        h = 2 * i
        after = scores(q_of(h + 1), chunks, s1)
        stats = one(h, s0, top, stats)
        top = scores(q_of(jnp.minimum(h + 2, GROUP - 1)), chunks, s0)
        return top, one(h + 1, s1, after, stats)

    first = scores(q_of(0), chunks, s0)
    l_ref[...] = lax.fori_loop(0, GROUP // 2, pair, (first, jnp.zeros(l_ref.shape, F32)), unroll=2)[1]


def state_shapes(rows):
    return [jax.ShapeDtypeStruct((rows, GROUP * HD), F32), jax.ShapeDtypeStruct((rows, HD), F32)]


def heads_scratch(rows, count):
    return [pltpu.VMEM((count, 2 * HD), BF), pltpu.VMEM((rows, count), F32), pltpu.VMEM((rows, count), F32)]


def start_body(idx, q_ref, k_ref, v_ref, o_ref, l_ref, *scratch):
    del idx
    heads_body([k_ref], [v_ref], q_ref, None, o_ref, l_ref, *scratch)


def attend_start(idx, q_all, keys, values):
    rows, count = q_all.shape[0], keys.shape[0]
    whole = lambda shape: pl.BlockSpec(shape, lambda i, idx: (0, 0))
    return pl.pallas_call(
        start_body,
        out_shape=state_shapes(rows),
        grid_spec=pltpu.PrefetchScalarGridSpec(
            num_scalar_prefetch=1,
            grid=(1,),
            in_specs=[
                whole(q_all.shape),
                pl.BlockSpec((count, HD), lambda i, idx: (0, idx[1])),
                pl.BlockSpec((count, HD), lambda i, idx: (0, idx[1])),
            ],
            out_specs=[whole(v.shape) for v in state_shapes(rows)],
            scratch_shapes=heads_scratch(rows, count),
        ),
        compiler_params=params(24),
        name="attend_start",
    )(idx, q_all, keys, values)


def more_body(q_ref, so_ref, sl_ref, b_ref, c_ref, o_ref, l_ref, *scratch):
    n = b_ref.shape[0] // 2
    keys, values = [[r.at[at] for r in (b_ref, c_ref)] for at in (pl.ds(0, n), pl.ds(n, n))]
    heads_body(keys, values, q_ref, (so_ref, sl_ref), o_ref, l_ref, *scratch)


def attend_more(q_all, state, parts):
    rows = q_all.shape[0]
    return pl.pallas_call(
        more_body,
        out_shape=state_shapes(rows),
        scratch_shapes=heads_scratch(rows, parts[0].shape[0]),
        compiler_params=params(24),
        name="attend_more",
    )(q_all, *state, *parts)


def last_body(own, idx, q_ref, so_ref, sl_ref, b_ref, *rest):
    n = b_ref.shape[0] // 2
    chunks, values = [(b_ref[:n, :], None)], [b_ref[n:, :]]
    if own:
        par_ref, sk_ref, sv_ref, o_ref, v1, s0, s1 = rest
        chunks.append((sk_ref[...], visible_rows(par_ref[...])))
        values.append(sv_ref[...])
    else:
        o_ref, v1, s0, s1 = rest
    with_ones(v1, values)
    rows = q_ref.shape[0]
    lane = lax.broadcasted_iota(jnp.int32, (rows, HD), 1)
    stats = jnp.zeros((rows, HD), F32)
    tops = [scores(q_ref[:, h * HD : (h + 1) * HD], chunks, s) for h, s in enumerate((s0, s1))]
    for h, s in enumerate((s0, s1)):
        cols = slice(h * HD, (h + 1) * HD)
        state = so_ref[:, cols], lane_of(sl_ref[...], 2 * idx[0] + h)
        o, lse = weigh(s, v1, tops[h], state)
        o_ref[:rows, cols] = o.astype(BF)
        left = lse
        for part in range(3):
            piece = left.astype(BF).astype(F32)
            left = left - piece
            stats = jnp.where(lane == 3 * h + part, piece, stats)
    o_ref[rows:, :] = stats.T[:16, :].astype(BF)


def attend_last(own, idx, q_all, state, part, extra):
    rows = q_all.shape[0]
    whole = lambda shape: pl.BlockSpec(shape, lambda i, idx: (0, 0))
    pair = pl.BlockSpec((rows, 2 * HD), lambda i, idx: (0, idx[0]))
    specs = [pair, pair, whole((rows, HD)), whole(part.shape)]
    args = [q_all, *state, part]
    count = part.shape[0] // 2
    if own:
        at = GROUP
        specs += [
            whole((rows, 1)),
            pl.BlockSpec((rows, HD), lambda i, idx: (0, at)),
            pl.BlockSpec((rows, HD), lambda i, idx: (0, at + 1)),
        ]
        args += [extra, q_all, q_all]
        count += rows
    return pl.pallas_call(
        lambda *refs: last_body(own, *refs),
        out_shape=jax.ShapeDtypeStruct((rows + 16, 2 * HD), BF),
        grid_spec=pltpu.PrefetchScalarGridSpec(
            num_scalar_prefetch=1,
            grid=(1,),
            in_specs=specs,
            out_specs=whole((rows + 16, 2 * HD)),
            scratch_shapes=heads_scratch(rows, count),
        ),
        compiler_params=params(24),
        name="attend_own" if own else "attend_last",
    )(idx, *args)


def combine(parts, att):
    rows = att.shape[0]
    r = lax.broadcasted_iota(jnp.int32, (rows, rows), 0)
    c = lax.broadcasted_iota(jnp.int32, (rows, rows), 1)
    eye = (r == c).astype(F32).astype(BF)
    stats = [nt(eye, p[rows:, :]) for p in parts]
    for h in range(2):
        at = 3 * h
        lse = [s[:, at : at + 1] + s[:, at + 1 : at + 2] + s[:, at + 2 : at + 3] for s in stats]
        top = jnp.maximum(jnp.maximum(lse[0], lse[1]), jnp.maximum(lse[2], lse[3]))
        w = [jnp.exp2(v - top) for v in lse]
        inv = 1.0 / (w[0] + w[1] + w[2] + w[3])
        cols = slice(h * HD, (h + 1) * HD)
        acc = sum(p[:rows, cols].astype(F32) * (v * inv) for p, v in zip(parts, w))
        att[:, cols] = acc.astype(BF)


def project_body(*refs):
    *parts, w_ref, o_ref, att = refs

    @pl.when(pl.program_id(0) == 0)
    def _():
        combine(parts, att)

    o_ref[...] = mm(att[...], w_ref[...]).astype(BF)


def project(parts, weights, steps=4):
    rows, width = parts[0].shape[0] - 16, weights.shape[1]
    return pl.pallas_call(
        project_body,
        out_shape=pltpu.HBM((rows, width), BF),
        grid=(steps,),
        in_specs=[
            *[pl.BlockSpec(parts[0].shape, lambda i: (0, 0))] * 4,
            pl.BlockSpec((weights.shape[0], width // steps), lambda i: (0, i)),
        ],
        out_specs=pl.BlockSpec((rows, width // steps), lambda i: (0, i)),
        scratch_shapes=[pltpu.VMEM((rows, 2 * HD), BF)],
        compiler_params=params(24),
        name="project",
    )(*parts, weights)


def route_body(p_ref, res_ref, gain_ref, router_ref, hot_ref, sel_ref, pack_ref, mixed_ref, gates_ref, buf, router_buf, sem):
    fetch = pltpu.make_async_copy(router_ref, router_buf, sem.at[4])
    fetch.start()
    rows, width = res_ref.shape
    step = width // CHUNK
    kept = []
    for c in range(CHUNK):
        cols = slice(c * step, (c + 1) * step)
        acc = res_ref[:, cols].astype(F32)
        for j in range(p_ref.shape[0] // rows):
            acc = acc + p_ref[j * rows : (j + 1) * rows, cols].astype(F32)
        mixed_ref[:, cols] = acc
        kept.append(acc)
    square = sum(jnp.sum(a * a, axis=1, keepdims=True) for a in kept)
    inverse = lax.rsqrt(square / width + EPSILON)
    normed = [(a * inverse * gain_ref[:, c * step : (c + 1) * step]).astype(BF) for c, a in enumerate(kept)]
    rows = jnp.concatenate(normed, axis=0)
    pieces = pack_ref.shape[0] // 4
    copies = []
    for j in range(4):
        at = pl.ds(j * pieces, pieces)
        buf[at, :] = mm(sel_ref[at, :], rows).astype(BF)
        copies.append(pltpu.make_async_copy(buf.at[at], pack_ref.at[at], sem.at[j]))
        copies[-1].start()
    fetch.wait()
    logits = sum(mm(n, router_buf[c * step : (c + 1) * step, :]) for c, n in enumerate(normed))
    sig = hot_ref[...] * jax.nn.sigmoid(logits)
    gates_ref[...] = sig / jnp.sum(sig, axis=1, keepdims=True)
    for copy in copies:
        copy.wait()


def route(partial, residual, gain, router, hot, select):
    rows, width = residual.shape
    step = width // CHUNK
    experts = router.shape[1]
    whole = lambda shape: pl.BlockSpec(shape, lambda i: (0, 0))
    router = pltpu.with_memory_space_constraint(router, pltpu.HBM)
    args = (partial, residual, gain, router, hot, select)
    return pl.pallas_call(
        route_body,
        out_shape=(
            pltpu.HBM((select.shape[0], step), BF),
            jax.ShapeDtypeStruct((rows, width), F32),
            jax.ShapeDtypeStruct((rows, experts), F32),
        ),
        grid=(1,),
        in_specs=[pl.BlockSpec(memory_space=pltpu.HBM) if v is router else whole(v.shape) for v in args],
        out_specs=(
            pl.BlockSpec(memory_space=pltpu.HBM),
            whole((rows, width)),
            whole((rows, experts)),
        ),
        scratch_shapes=[
            pltpu.VMEM((select.shape[0], step), BF),
            pltpu.VMEM(router.shape, BF),
            pltpu.SemaphoreType.DMA((5,)),
        ],
        compiler_params=params(),
        name="route",
    )(*args)


def shuffle_matrix():
    n = 16 * CAP * CHUNK
    to = lax.broadcasted_iota(jnp.int32, (n, n), 0)
    come = lax.broadcasted_iota(jnp.int32, (n, n), 1)
    tokens = 16 * CAP
    chunk = come % CHUNK
    token = come // CHUNK
    return (to == chunk * tokens + token).astype(F32).astype(BF)


STEPS = 4


def expert_body(perm_ref, back_ref, x_in, g_hbm, u_hbm, d_hbm, o_hbm, x, g, u, d, act, y, out, sems, out_sems):
    block = perm_ref.shape[0]
    tokens = block // CHUNK
    depth = g.shape[1]
    span = d.shape[2]
    count = x_in.shape[0] // block
    fetch = []
    for k in range(STEPS):
        for j, (src, dst) in enumerate(((g_hbm, g), (u_hbm, u))):
            at = pl.ds(k * depth, depth)
            fetch.append(pltpu.make_async_copy(src.at[at, :], dst.at[k], sems.at[2 * k + j]))
    for k in range(STEPS):
        at = pl.ds(k * span, span)
        fetch.append(pltpu.make_async_copy(d_hbm.at[:, at], d.at[k], sems.at[2 * STEPS + k]))
    for copy in fetch:
        copy.start()
    step = x_in.shape[1]
    for b in range(count):
        z = mm(perm_ref[...], x_in[b * block : (b + 1) * block, :]).astype(BF)
        for c in range(CHUNK):
            x[b * tokens : (b + 1) * tokens, c * step : (c + 1) * step] = z[c * tokens : (c + 1) * tokens, :]
    gate = up = None
    for k in range(STEPS):
        piece = x[:, k * depth : (k + 1) * depth]
        fetch[2 * k].wait()
        part = mm(piece, g[k])
        gate = part if gate is None else gate + part
        fetch[2 * k + 1].wait()
        part = mm(piece, u[k])
        up = part if up is None else up + part
    act[...] = (jax.nn.silu(gate) * up).astype(BF)
    for k in range(STEPS):
        fetch[2 * STEPS + k].wait()
        y[:, k * span : (k + 1) * span] = mm(act[...], d[k]).astype(BF)
    sends = []
    for b in range(count):
        rows = slice(b * tokens, (b + 1) * tokens)
        z = jnp.concatenate([y[rows, c * step : (c + 1) * step] for c in range(CHUNK)], axis=0)
        at = pl.ds(b * block, block)
        out[at, :] = mm(back_ref[...], z).astype(BF)
        sends.append(pltpu.make_async_copy(out.at[at], o_hbm.at[at], out_sems.at[b]))
        sends[-1].start()
    for copy in sends:
        copy.wait()


def expert(arrived, perm, back, gate_w, up_w, down_w):
    width, hidden = gate_w.shape
    total, step = arrived.shape
    tokens = total // CHUNK
    blocks = total // perm.shape[0]
    whole = lambda shape: pl.BlockSpec(shape, lambda i: (0, 0))
    hbm = pl.BlockSpec(memory_space=pltpu.HBM)
    return pl.pallas_call(
        expert_body,
        out_shape=pltpu.HBM(arrived.shape, BF),
        grid=(1,),
        in_specs=[whole(perm.shape), whole(back.shape), whole(arrived.shape), hbm, hbm, hbm],
        out_specs=hbm,
        scratch_shapes=[
            pltpu.VMEM((tokens, width), BF),
            pltpu.VMEM((STEPS, width // STEPS, hidden), BF),
            pltpu.VMEM((STEPS, width // STEPS, hidden), BF),
            pltpu.VMEM((STEPS, hidden, width // STEPS), BF),
            pltpu.VMEM((tokens, hidden), BF),
            pltpu.VMEM((tokens, width), BF),
            pltpu.VMEM((total, step), BF),
            pltpu.SemaphoreType.DMA((3 * STEPS,)),
            pltpu.SemaphoreType.DMA((blocks,)),
        ],
        compiler_params=params(),
        name="expert",
    )(perm, back, arrived, gate_w, up_w, down_w)


def finish_body(ret_ref, mask_ref, gates_ref, mixed_ref, o_ref):
    rows, experts = gates_ref.shape
    span = ret_ref.shape[0]
    step = ret_ref.shape[1]
    e = lax.broadcasted_iota(jnp.int32, (experts, span), 0)
    at = lax.broadcasted_iota(jnp.int32, (experts, span), 1)
    spread = (e == at // (span // experts)).astype(F32).astype(BF)
    high, low = hi_lo(gates_ref[...])
    wide = mm(high, spread) + mm(low, spread)
    weights = jnp.concatenate([wide] * CHUNK, axis=0) * mask_ref[...].astype(F32)
    high, low = hi_lo(weights)
    moe = mm(high, ret_ref[...]) + mm(low, ret_ref[...])
    for c in range(CHUNK):
        cols = slice(c * step, (c + 1) * step)
        o_ref[:, cols] = (mixed_ref[:, cols] + moe[c * rows : (c + 1) * rows, :]).astype(BF)


def finish(returned, mask, gates, mixed):
    return pl.pallas_call(
        finish_body,
        out_shape=jax.ShapeDtypeStruct(mixed.shape, BF),
        compiler_params=params(),
        name="finish",
    )(returned, mask, gates, mixed)


def ready_body(q_hbm, k_hbm, v_hbm, o_ref, q_ref, k_ref, v_ref, sems):
    fetch = [
        pltpu.make_async_copy(src, dst, sems.at[i])
        for i, (src, dst) in enumerate(((q_hbm, q_ref), (k_hbm, k_ref), (v_hbm, v_ref)))
    ]
    for copy in fetch:
        copy.start()
    for copy in fetch:
        copy.wait()
    rows, side = q_ref.shape[0], KVH
    across = o_ref.shape[0] // rows // side
    wide = q_ref.shape[1] // side
    for z in range(side):
        for x in range(across):
            at = slice((z * across + x) * rows, (z * across + x + 1) * rows)
            o_ref[at, :wide] = q_ref[:, z * wide : (z + 1) * wide]
            o_ref[at, wide : wide + HD] = k_ref[:, z * HD : (z + 1) * HD]
            o_ref[at, wide + HD :] = v_ref[:, z * HD : (z + 1) * HD]


def ready(*arrays, devices):
    rows = arrays[0].shape[0]
    arrays = [pltpu.with_memory_space_constraint(a, pltpu.HBM) for a in arrays]
    shape = (devices * rows, (GROUP + 2) * HD)
    return pl.pallas_call(
        ready_body,
        out_shape=pltpu.HBM(shape, BF),
        grid=(1,),
        in_specs=[pl.BlockSpec(memory_space=pltpu.HBM)] * len(arrays),
        out_specs=pl.BlockSpec(shape, lambda i: (0, 0)),
        scratch_shapes=[*[pltpu.VMEM(a.shape, BF) for a in arrays], pltpu.SemaphoreType.DMA((len(arrays),))],
        compiler_params=params(24),
        name="ready",
    )(*arrays)


def local(
    queries,
    prefix_keys,
    prefix_values,
    suffix_keys,
    suffix_values,
    parents,
    out_proj,
    residual,
    norm_gain,
    router,
    routes,
    expert_gate,
    expert_up,
    expert_down,
):
    seq_count = lax.axis_size("seq")
    side = KVH
    across = seq_count // side
    s = lax.axis_index("seq")
    z, x = s // across, s % across
    q, sk, sv = queries[0], suffix_keys[0], suffix_values[0]
    rows = q.shape[0]
    keys, values = prefix_keys[0], prefix_values[0]
    copies = ready(q, sk, sv, devices=seq_count)
    parts = []
    for d in (1, 3, 2):
        head = (z + d) % side
        piece = jnp.concatenate(
            [lax.dynamic_slice_in_dim(a, head * HD, HD, 1) for a in (keys, values)], axis=0
        )
        parts.append(lax.ppermute(piece, "seq", [(i, (i + d * across) % seq_count) for i in range(seq_count)]))
    q_all = lax.all_to_all(copies.reshape(seq_count, rows, -1), "seq", 0, 0, tiled=True)
    q_all = q_all.reshape(copies.shape)
    place = jnp.stack([x, z]).astype(jnp.int32)
    state = attend_start(place, q_all, keys, values)
    state = attend_more(q_all, state, parts[:2])
    along_x = lambda a, d: lax.ppermute(
        a, "seq", [(i, i // across * across + (i + d) % across) for i in range(seq_count)]
    )
    blocks = []
    for d in (2, 1, 3, 0):
        idx = jnp.stack([(x + d) % across, z]).astype(jnp.int32)
        block = attend_last(d == 0, idx, q_all, state, parts[2], parents[0][:, None])
        blocks.append(along_x(block, d) if d else block)
    projected = project(blocks, out_proj)
    arrived = lax.all_to_all(
        projected.reshape(seq_count, rows, -1), "seq", 0, 0, tiled=True
    ).reshape(projected.shape)
    experts = router.shape[1]
    ids = routes[0]
    hot = jnp.any(ids[:, :, None] == jnp.arange(experts, dtype=jnp.int32), axis=1)
    before = jnp.cumsum(hot.astype(jnp.int32), axis=0) - hot
    slots = hot[:, :, None] & (before[:, :, None] == jnp.arange(CAP, dtype=jnp.int32))
    same = jnp.eye(CHUNK, dtype=jnp.bool_)
    mask = slots[None, :, :, :, None] & same[:, None, None, None, :]
    mask = mask.reshape(CHUNK * rows, experts * CAP * CHUNK).astype(BF)
    chosen = jnp.moveaxis(slots, 0, 2)
    select = chosen[:, :, None, None, :] & same[None, None, :, :, None]
    select = select.reshape(experts * CAP * CHUNK, CHUNK * rows).astype(BF)
    packed, mixed, gates = route(arrived, residual[0], norm_gain[None, :], router, hot.astype(F32), select)
    exchange = lambda a: lax.all_to_all(
        a.reshape(experts, CAP * CHUNK, -1), ("seq", "grp"), 0, 0, tiled=True
    ).reshape(a.shape)
    order = shuffle_matrix()
    finished = expert(exchange(packed), order, order.T, expert_gate[0], expert_up[0], expert_down[0])
    return finish(exchange(finished), mask, gates, mixed)[None]


def solution(mesh):
    rows = P("grp", "seq", None)
    spread = P(("seq", "grp"), None, None)
    in_specs = (
        rows, rows, rows, rows, rows, P("grp", None), P("seq", None), rows, P(), P(), rows, spread, spread, spread,
    )

    return jax.shard_map(local, mesh=mesh, in_specs=in_specs, out_specs=rows, check_vma=False)
```

```python
import math

import jax
import jax.numpy as jnp
from jax import lax
from jax.experimental import pallas as pl
from jax.experimental.pallas import tpu as pltpu
from jax.sharding import PartitionSpec as P


HEADS = 32
KVH = 4
HD = 128
EPSILON = 1e-06
GROUP = HEADS // KVH
C2 = HD ** (-0.5) * math.log2(math.e)
CAP = 2
CHUNK = 8
BF = jnp.bfloat16
F32 = jnp.float32


def params(mib=48, semantics=None):
    return pltpu.CompilerParams(
        vmem_limit_bytes=mib << 20, dimension_semantics=semantics
    )


def nt(a, b):
    return lax.dot_general(a, b, (((1,), (1,)), ((), ())), preferred_element_type=F32)


def mm(a, b):
    return jnp.dot(a, b, preferred_element_type=F32)


def hi_lo(x):
    hi = x.astype(BF)
    return hi, (x - hi.astype(F32)).astype(BF)


def scores(q, chunks, s_ref):
    top, at = None, 0
    for k, visible in chunks:
        s = nt(q, k) * C2
        if visible is not None:
            s = jnp.where(visible, s, -1e30)
        s_ref[:, at : at + k.shape[0]] = s
        m = jnp.max(s, axis=1, keepdims=True)
        top = m if top is None else jnp.maximum(top, m)
        at += k.shape[0]
    return top


def weigh(s_ref, values, top, state, span=512):
    if state is not None:
        before, lse = state
        top = jnp.maximum(top, lse)
    acc = None
    for at in range(0, s_ref.shape[1], span):
        cols = slice(at, min(at + span, s_ref.shape[1]))
        part = mm(jnp.exp2(s_ref[:, cols] - top).astype(BF), values[cols, :])
        acc = part if acc is None else acc + part
    out, total = acc[:, :HD], acc[:, HD : HD + 1]
    if state is not None:
        a = jnp.exp2(lse - top)
        out, total = out + before * a, total + a
    return out / total, top + jnp.log2(total)


def with_ones(ref, values):
    at = 0
    for v in values:
        ref[at : at + v.shape[0], :HD] = v
        ref[at : at + v.shape[0], HD:] = jnp.ones(v.shape, BF)
        at += v.shape[0]


def lane_of(stats, h):
    lane = lax.broadcasted_iota(jnp.int32, stats.shape, 1)
    return jnp.sum(jnp.where(lane == h, stats, 0.0), axis=1, keepdims=True)


def visible_rows(par_ref):
    n = par_ref.shape[0]
    rows = lax.broadcasted_iota(jnp.int32, (n, n), 0)
    cols = lax.broadcasted_iota(jnp.int32, (n, n), 1)
    side = n // 4
    block = side // 4
    starts = [z * side + x * block for x in range(4) for z in range(4)]
    parents = jnp.concatenate([par_ref[at : at + block, :] for at in starts], axis=0)
    number = cols // block % 4 * side + cols // side * block + cols % block
    step = ((parents == number).astype(F32) + (rows == cols).astype(F32)).astype(BF)
    two = mm(step, step).astype(BF)
    four = mm(two, two).astype(BF)
    six = mm(four, two).astype(BF)
    return mm(six, step) > 0.5


def heads_body(k_refs, v_refs, q_ref, before, o_ref, l_ref, v1, s0, s1):
    chunks = [(r[...], None) for r in k_refs]
    with_ones(v1, [r[...] for r in v_refs])

    def q_of(h):
        return q_ref[:, pl.ds(pl.multiple_of(h * HD, HD), HD)]

    def one(h, s_ref, top, stats):
        cols = pl.ds(pl.multiple_of(h * HD, HD), HD)
        state = None if before is None else (before[0][:, cols], lane_of(before[1][...], h))
        o, lse = weigh(s_ref, v1, top, state)
        o_ref[:, cols] = o
        lane = lax.broadcasted_iota(jnp.int32, stats.shape, 1)
        return jnp.where(lane == h, lse, stats)

    def pair(i, carry):
        top, stats = carry
        h = 2 * i
        after = scores(q_of(h + 1), chunks, s1)
        stats = one(h, s0, top, stats)
        top = scores(q_of(jnp.minimum(h + 2, GROUP - 1)), chunks, s0)
        return top, one(h + 1, s1, after, stats)

    first = scores(q_of(0), chunks, s0)
    l_ref[...] = lax.fori_loop(0, GROUP // 2, pair, (first, jnp.zeros(l_ref.shape, F32)), unroll=2)[1]


def state_shapes(rows):
    return [jax.ShapeDtypeStruct((rows, GROUP * HD), F32), jax.ShapeDtypeStruct((rows, HD), F32)]


def heads_scratch(rows, count):
    return [pltpu.VMEM((count, 2 * HD), BF), pltpu.VMEM((rows, count), F32), pltpu.VMEM((rows, count), F32)]


def start_body(idx, q_ref, k_ref, v_ref, o_ref, l_ref, *scratch):
    del idx
    heads_body([k_ref], [v_ref], q_ref, None, o_ref, l_ref, *scratch)


def attend_start(idx, q_all, keys, values):
    rows, count = q_all.shape[0], keys.shape[0]
    whole = lambda shape: pl.BlockSpec(shape, lambda i, idx: (0, 0))
    return pl.pallas_call(
        start_body,
        out_shape=state_shapes(rows),
        grid_spec=pltpu.PrefetchScalarGridSpec(
            num_scalar_prefetch=1,
            grid=(1,),
            in_specs=[
                whole(q_all.shape),
                pl.BlockSpec((count, HD), lambda i, idx: (0, idx[1])),
                pl.BlockSpec((count, HD), lambda i, idx: (0, idx[1])),
            ],
            out_specs=[whole(v.shape) for v in state_shapes(rows)],
            scratch_shapes=heads_scratch(rows, count),
        ),
        compiler_params=params(24),
        name="attend_start",
    )(idx, q_all, keys, values)


def more_body(q_ref, so_ref, sl_ref, b_ref, c_ref, o_ref, l_ref, *scratch):
    n = b_ref.shape[0] // 2
    keys, values = [[r.at[at] for r in (b_ref, c_ref)] for at in (pl.ds(0, n), pl.ds(n, n))]
    heads_body(keys, values, q_ref, (so_ref, sl_ref), o_ref, l_ref, *scratch)


def attend_more(q_all, state, parts):
    rows = q_all.shape[0]
    return pl.pallas_call(
        more_body,
        out_shape=state_shapes(rows),
        scratch_shapes=heads_scratch(rows, parts[0].shape[0]),
        compiler_params=params(24),
        name="attend_more",
    )(q_all, *state, *parts)


def last_body(shifts, idx, q_ref, so_ref, sl_ref, b_ref, *rest):
    n = b_ref.shape[0] // 2
    chunks, values = [(b_ref[:n, :], None)], [b_ref[n:, :]]
    if shifts == (0,):
        par_ref, sk_ref, sv_ref, *rest = rest
        chunks.append((sk_ref[...], visible_rows(par_ref)))
        values.append(sv_ref[...])
    outs, (v1, *held) = rest[: len(shifts)], rest[len(shifts) :]
    with_ones(v1, values)
    rows = q_ref.shape[0]
    lane = lax.broadcasted_iota(jnp.int32, (rows, HD), 1)
    heads = [(idx[0] + d) % (GROUP // 2) * 2 + h for d in shifts for h in range(2)]
    columns = [pl.ds(pl.multiple_of(h * HD, HD), HD) for h in heads]
    tops = {0: scores(q_ref[:, columns[0]], chunks, held[0])}
    for i, (head, cols) in enumerate(zip(heads, columns)):
        if i + 1 < len(heads):
            tops[i + 1] = scores(q_ref[:, columns[i + 1]], chunks, held[(i + 1) % len(held)])
        state = so_ref[:, cols], lane_of(sl_ref[...], head)
        o, lse = weigh(held[i % len(held)], v1, tops[i], state)
        h, o_ref = i % 2, outs[i // 2]
        stats = jnp.zeros((rows, HD), F32) if h == 0 else stats
        o_ref[:rows, h * HD : (h + 1) * HD] = o.astype(BF)
        left = lse
        for part in range(3):
            piece = left.astype(BF).astype(F32)
            left = left - piece
            stats = jnp.where(lane == 3 * h + part, piece, stats)
        if h == 1:
            o_ref[rows:, :] = stats.T[:16, :].astype(BF)


def attend_last(shifts, idx, q_all, state, part, extra):
    rows = q_all.shape[0]
    whole = lambda shape: pl.BlockSpec(shape, lambda i, idx: (0, 0))
    args = [q_all, *state, part]
    specs = [whole(v.shape) for v in args]
    count = part.shape[0] // 2
    if shifts == (0,):
        at = GROUP
        specs += [
            whole((rows, 1)),
            pl.BlockSpec((rows, HD), lambda i, idx: (0, at)),
            pl.BlockSpec((rows, HD), lambda i, idx: (0, at + 1)),
        ]
        args += [extra, q_all, q_all]
        count += rows
    shape = (rows + 16, 2 * HD)
    return pl.pallas_call(
        lambda *refs: last_body(shifts, *refs),
        out_shape=[jax.ShapeDtypeStruct(shape, BF)] * len(shifts),
        grid_spec=pltpu.PrefetchScalarGridSpec(
            num_scalar_prefetch=1,
            grid=(1,),
            in_specs=specs,
            out_specs=[whole(shape)] * len(shifts),
            scratch_shapes=[pltpu.VMEM((count, 2 * HD), BF), *[pltpu.VMEM((rows, count), F32)] * 2],
        ),
        compiler_params=params(24),
        name="attend_own" if shifts == (0,) else "attend_last",
    )(idx, *args)


def combine(parts, att):
    rows = att.shape[0]
    r = lax.broadcasted_iota(jnp.int32, (rows, rows), 0)
    c = lax.broadcasted_iota(jnp.int32, (rows, rows), 1)
    eye = (r == c).astype(F32).astype(BF)
    stats = [nt(eye, p[rows:, :]) for p in parts]
    for h in range(2):
        at = 3 * h
        lse = [s[:, at : at + 1] + s[:, at + 1 : at + 2] + s[:, at + 2 : at + 3] for s in stats]
        top = jnp.maximum(jnp.maximum(lse[0], lse[1]), jnp.maximum(lse[2], lse[3]))
        w = [jnp.exp2(v - top) for v in lse]
        inv = 1.0 / (w[0] + w[1] + w[2] + w[3])
        cols = slice(h * HD, (h + 1) * HD)
        acc = sum(p[:rows, cols].astype(F32) * (v * inv) for p, v in zip(parts, w))
        att[:, cols] = acc.astype(BF)


def project_body(*refs):
    *parts, w_ref, o_ref, mixed_rows, att = refs

    @pl.when(pl.program_id(0) == 0)
    def _():
        combine(parts, mixed_rows)
        side = att.shape[0] // 4
        block = side // 4
        for z in range(4):
            for x in range(4):
                to, come = z * side + x * block, x * side + z * block
                att[to : to + block, :] = mixed_rows[come : come + block, :]

    o_ref[...] = mm(att[...], w_ref[...]).astype(BF)


def project(parts, weights, steps=4):
    rows, width = parts[0].shape[0] - 16, weights.shape[1]
    return pl.pallas_call(
        project_body,
        out_shape=pltpu.HBM((rows, width), BF),
        grid=(steps,),
        in_specs=[
            *[pl.BlockSpec(parts[0].shape, lambda i: (0, 0))] * 4,
            pl.BlockSpec((weights.shape[0], width // steps), lambda i: (0, i)),
        ],
        out_specs=pl.BlockSpec((rows, width // steps), lambda i: (0, i)),
        scratch_shapes=[pltpu.VMEM((rows, 2 * HD), BF), pltpu.VMEM((rows, 2 * HD), BF)],
        compiler_params=params(24),
        name="project",
    )(*parts, weights)


def route_body(p_ref, res_ref, gain_ref, router_ref, hot_ref, sel_ref, pack_ref, mixed_ref, gates_ref, buf, router_buf, sem):
    fetch = pltpu.make_async_copy(router_ref, router_buf, sem.at[4])
    fetch.start()
    rows, width = res_ref.shape
    step = width // CHUNK
    kept = []
    for c in range(CHUNK):
        cols = slice(c * step, (c + 1) * step)
        acc = res_ref[:, cols].astype(F32)
        for j in range(p_ref.shape[0] // rows):
            acc = acc + p_ref[j * rows : (j + 1) * rows, cols].astype(F32)
        mixed_ref[:, cols] = acc
        kept.append(acc)
    square = sum(jnp.sum(a * a, axis=1, keepdims=True) for a in kept)
    inverse = lax.rsqrt(square / width + EPSILON)
    normed = [(a * inverse * gain_ref[:, c * step : (c + 1) * step]).astype(BF) for c, a in enumerate(kept)]
    rows = jnp.concatenate(normed, axis=0)
    pieces = pack_ref.shape[0] // 4
    copies = []
    for j in range(4):
        at = pl.ds(j * pieces, pieces)
        buf[at, :] = mm(sel_ref[at, :], rows).astype(BF)
        copies.append(pltpu.make_async_copy(buf.at[at], pack_ref.at[at], sem.at[j]))
        copies[-1].start()
    fetch.wait()
    logits = sum(mm(n, router_buf[c * step : (c + 1) * step, :]) for c, n in enumerate(normed))
    sig = hot_ref[...] * jax.nn.sigmoid(logits)
    gates_ref[...] = sig / jnp.sum(sig, axis=1, keepdims=True)
    for copy in copies:
        copy.wait()


def route(partial, residual, gain, router, hot, select):
    rows, width = residual.shape
    step = width // CHUNK
    experts = router.shape[1]
    whole = lambda shape: pl.BlockSpec(shape, lambda i: (0, 0))
    router = pltpu.with_memory_space_constraint(router, pltpu.HBM)
    args = (partial, residual, gain, router, hot, select)
    return pl.pallas_call(
        route_body,
        out_shape=(
            pltpu.HBM((select.shape[0], step), BF),
            jax.ShapeDtypeStruct((rows, width), F32),
            jax.ShapeDtypeStruct((rows, experts), F32),
        ),
        grid=(1,),
        in_specs=[pl.BlockSpec(memory_space=pltpu.HBM) if v is router else whole(v.shape) for v in args],
        out_specs=(
            pl.BlockSpec(memory_space=pltpu.HBM),
            whole((rows, width)),
            whole((rows, experts)),
        ),
        scratch_shapes=[
            pltpu.VMEM((select.shape[0], step), BF),
            pltpu.VMEM(router.shape, BF),
            pltpu.SemaphoreType.DMA((5,)),
        ],
        compiler_params=params(),
        name="route",
    )(*args)


def shuffle_matrix():
    n = 16 * CAP * CHUNK
    to = lax.broadcasted_iota(jnp.int32, (n, n), 0)
    come = lax.broadcasted_iota(jnp.int32, (n, n), 1)
    tokens = 16 * CAP
    chunk = come % CHUNK
    token = come // CHUNK
    return (to == chunk * tokens + token).astype(F32).astype(BF)


STEPS = 4


def expert_body(perm_ref, back_ref, x_in, g_hbm, u_hbm, d_hbm, o_hbm, x, g, u, d, act, y, out, sems, out_sems):
    block = perm_ref.shape[0]
    tokens = block // CHUNK
    depth = g.shape[1]
    span = d.shape[2]
    count = x_in.shape[0] // block
    fetch = []
    for k in range(STEPS):
        for j, (src, dst) in enumerate(((g_hbm, g), (u_hbm, u))):
            at = pl.ds(k * depth, depth)
            fetch.append(pltpu.make_async_copy(src.at[at, :], dst.at[k], sems.at[2 * k + j]))
    for k in range(STEPS):
        at = pl.ds(k * span, span)
        fetch.append(pltpu.make_async_copy(d_hbm.at[:, at], d.at[k], sems.at[2 * STEPS + k]))
    for copy in fetch:
        copy.start()
    step = x_in.shape[1]
    for b in range(count):
        z = mm(perm_ref[...], x_in[b * block : (b + 1) * block, :]).astype(BF)
        for c in range(CHUNK):
            x[b * tokens : (b + 1) * tokens, c * step : (c + 1) * step] = z[c * tokens : (c + 1) * tokens, :]
    gate = up = None
    for k in range(STEPS):
        piece = x[:, k * depth : (k + 1) * depth]
        fetch[2 * k].wait()
        part = mm(piece, g[k])
        gate = part if gate is None else gate + part
        fetch[2 * k + 1].wait()
        part = mm(piece, u[k])
        up = part if up is None else up + part
    act[...] = (jax.nn.silu(gate) * up).astype(BF)
    for k in range(STEPS):
        fetch[2 * STEPS + k].wait()
        y[:, k * span : (k + 1) * span] = mm(act[...], d[k]).astype(BF)
    sends = []
    for b in range(count):
        rows = slice(b * tokens, (b + 1) * tokens)
        z = jnp.concatenate([y[rows, c * step : (c + 1) * step] for c in range(CHUNK)], axis=0)
        at = pl.ds(b * block, block)
        out[at, :] = mm(back_ref[...], z).astype(BF)
        sends.append(pltpu.make_async_copy(out.at[at], o_hbm.at[at], out_sems.at[b]))
        sends[-1].start()
    for copy in sends:
        copy.wait()


def expert(arrived, perm, back, gate_w, up_w, down_w):
    width, hidden = gate_w.shape
    total, step = arrived.shape
    tokens = total // CHUNK
    blocks = total // perm.shape[0]
    whole = lambda shape: pl.BlockSpec(shape, lambda i: (0, 0))
    hbm = pl.BlockSpec(memory_space=pltpu.HBM)
    return pl.pallas_call(
        expert_body,
        out_shape=pltpu.HBM(arrived.shape, BF),
        grid=(1,),
        in_specs=[whole(perm.shape), whole(back.shape), whole(arrived.shape), hbm, hbm, hbm],
        out_specs=hbm,
        scratch_shapes=[
            pltpu.VMEM((tokens, width), BF),
            pltpu.VMEM((STEPS, width // STEPS, hidden), BF),
            pltpu.VMEM((STEPS, width // STEPS, hidden), BF),
            pltpu.VMEM((STEPS, hidden, width // STEPS), BF),
            pltpu.VMEM((tokens, hidden), BF),
            pltpu.VMEM((tokens, width), BF),
            pltpu.VMEM((total, step), BF),
            pltpu.SemaphoreType.DMA((3 * STEPS,)),
            pltpu.SemaphoreType.DMA((blocks,)),
        ],
        compiler_params=params(),
        name="expert",
    )(perm, back, arrived, gate_w, up_w, down_w)


def finish_body(ret_ref, mask_ref, gates_ref, mixed_ref, o_ref):
    rows, experts = gates_ref.shape
    span = ret_ref.shape[0]
    step = ret_ref.shape[1]
    e = lax.broadcasted_iota(jnp.int32, (experts, span), 0)
    at = lax.broadcasted_iota(jnp.int32, (experts, span), 1)
    spread = (e == at // (span // experts)).astype(F32).astype(BF)
    high, low = hi_lo(gates_ref[...])
    wide = mm(high, spread) + mm(low, spread)
    weights = jnp.concatenate([wide] * CHUNK, axis=0) * mask_ref[...].astype(F32)
    high, low = hi_lo(weights)
    moe = mm(high, ret_ref[...]) + mm(low, ret_ref[...])
    for c in range(CHUNK):
        cols = slice(c * step, (c + 1) * step)
        o_ref[:, cols] = (mixed_ref[:, cols] + moe[c * rows : (c + 1) * rows, :]).astype(BF)


def finish(returned, mask, gates, mixed):
    return pl.pallas_call(
        finish_body,
        out_shape=jax.ShapeDtypeStruct(mixed.shape, BF),
        compiler_params=params(),
        name="finish",
    )(returned, mask, gates, mixed)


SHIFTS = (1, 3, 2)


def ready_body(idx, q_hbm, k_hbm, v_hbm, keys_hbm, values_hbm, o_ref, *rest):
    *pieces, q_ref, k_ref, v_ref, sems = rest
    fetch = [
        pltpu.make_async_copy(src, dst, sems.at[i])
        for i, (src, dst) in enumerate(((q_hbm, q_ref), (k_hbm, k_ref), (v_hbm, v_ref)))
    ]
    count = keys_hbm.shape[0]
    send = []
    for d, piece in zip(SHIFTS, pieces):
        cols = pl.ds(pl.multiple_of((idx[1] + d) % KVH * HD, HD), HD)
        for j, src in enumerate((keys_hbm, values_hbm)):
            to = piece.at[pl.ds(j * count, count), :]
            send.append(pltpu.make_async_copy(src.at[:, cols], to, sems.at[len(fetch) + len(send)]))
    for copy in fetch + send:
        copy.start()
    for copy in fetch:
        copy.wait()
    rows, wide = q_ref.shape[0], q_ref.shape[1] // KVH
    for z in range(KVH):
        at = slice(z * rows, (z + 1) * rows)
        o_ref[at, :wide] = q_ref[:, z * wide : (z + 1) * wide]
        o_ref[at, wide : wide + HD] = k_ref[:, z * HD : (z + 1) * HD]
        o_ref[at, wide + HD :] = v_ref[:, z * HD : (z + 1) * HD]
    for copy in send:
        copy.wait()


def ready(idx, *arrays):
    rows, count = arrays[0].shape[0], arrays[3].shape[0]
    arrays = [pltpu.with_memory_space_constraint(a, pltpu.HBM) for a in arrays]
    shape = (KVH * rows, (GROUP + 2) * HD)
    hbm = pl.BlockSpec(memory_space=pltpu.HBM)
    return pl.pallas_call(
        ready_body,
        out_shape=[pltpu.HBM(shape, BF), *[pltpu.HBM((2 * count, HD), BF)] * len(SHIFTS)],
        grid_spec=pltpu.PrefetchScalarGridSpec(
            num_scalar_prefetch=1,
            grid=(1,),
            in_specs=[hbm] * len(arrays),
            out_specs=[
                pl.BlockSpec(shape, lambda i, idx: (0, 0)),
                *[pl.BlockSpec((2 * count, HD), lambda i, idx: (0, 0))] * len(SHIFTS),
            ],
            scratch_shapes=[
                *[pltpu.VMEM(a.shape, BF) for a in arrays[:3]],
                pltpu.SemaphoreType.DMA((3 + 2 * len(SHIFTS),)),
            ],
        ),
        compiler_params=params(24),
        name="ready",
    )(idx, *arrays)


def local(
    queries,
    prefix_keys,
    prefix_values,
    suffix_keys,
    suffix_values,
    parents,
    out_proj,
    residual,
    norm_gain,
    router,
    routes,
    expert_gate,
    expert_up,
    expert_down,
):
    seq_count = lax.axis_size("seq")
    side = KVH
    across = seq_count // side
    s = lax.axis_index("seq")
    z, x = s // across, s % across
    q, sk, sv = queries[0], suffix_keys[0], suffix_values[0]
    rows = q.shape[0]
    keys, values = prefix_keys[0], prefix_values[0]
    place = jnp.stack([x, z]).astype(jnp.int32)
    copies, *pieces = ready(place, q, sk, sv, keys, values)
    parts = []
    for d, piece in zip(SHIFTS, pieces):
        parts.append(lax.ppermute(piece, "seq", [(i, (i + d * across) % seq_count) for i in range(seq_count)]))
    columns = [[i * across + j for i in range(side)] for j in range(across)]
    lines = [[i * across + j for j in range(across)] for i in range(side)]
    mine = lax.all_to_all(
        copies.reshape(side, rows, -1), "seq", 0, 0, tiled=True, axis_index_groups=columns
    ).reshape(copies.shape)
    q_all = lax.all_to_all(
        jnp.broadcast_to(mine, (across, *mine.shape)), "seq", 0, 0, tiled=True, axis_index_groups=lines
    )
    q_all = q_all.reshape(across * mine.shape[0], -1)
    state = attend_start(place, q_all, keys, values)
    state = attend_more(q_all, state, parts[:2])
    along_x = lambda a, d: lax.ppermute(
        a, "seq", [(i, i // across * across + (i + d) % across) for i in range(seq_count)]
    )
    others = (2, 1, 3)
    blocks = attend_last(others, place, q_all, state, parts[2], None)
    blocks = [along_x(block, d) for d, block in zip(others, blocks)]
    blocks += attend_last((0,), place, q_all, state, parts[2], parents[0][:, None])
    projected = project(blocks, out_proj)
    arrived = lax.all_to_all(
        projected.reshape(seq_count, rows, -1), "seq", 0, 0, tiled=True
    ).reshape(projected.shape)
    experts = router.shape[1]
    ids = routes[0]
    hot = jnp.any(ids[:, :, None] == jnp.arange(experts, dtype=jnp.int32), axis=1)
    before = jnp.cumsum(hot.astype(jnp.int32), axis=0) - hot
    slots = hot[:, :, None] & (before[:, :, None] == jnp.arange(CAP, dtype=jnp.int32))
    same = jnp.eye(CHUNK, dtype=jnp.bool_)
    mask = slots[None, :, :, :, None] & same[:, None, None, None, :]
    mask = mask.reshape(CHUNK * rows, experts * CAP * CHUNK).astype(BF)
    chosen = jnp.moveaxis(slots, 0, 2)
    select = chosen[:, :, None, None, :] & same[None, None, :, :, None]
    select = select.reshape(experts * CAP * CHUNK, CHUNK * rows).astype(BF)
    packed, mixed, gates = route(arrived, residual[0], norm_gain[None, :], router, hot.astype(F32), select)
    exchange = lambda a: lax.all_to_all(
        a.reshape(experts, CAP * CHUNK, -1), ("seq", "grp"), 0, 0, tiled=True
    ).reshape(a.shape)
    order = shuffle_matrix()
    finished = expert(exchange(packed), order, order.T, expert_gate[0], expert_up[0], expert_down[0])
    return finish(exchange(finished), mask, gates, mixed)[None]


def solution(mesh):
    rows = P("grp", "seq", None)
    spread = P(("seq", "grp"), None, None)
    in_specs = (
        rows, rows, rows, rows, rows, P("grp", None), P("seq", None), rows, P(), P(), rows, spread, spread, spread,
    )

    return jax.shard_map(local, mesh=mesh, in_specs=in_specs, out_specs=rows, check_vma=False)
```

```python
import math

import jax
import jax.numpy as jnp
from jax import lax
from jax.experimental import pallas as pl
from jax.experimental.pallas import tpu as pltpu
from jax.sharding import PartitionSpec as P


HEADS = 32
KVH = 4
HD = 128
EPSILON = 1e-06
GROUP = HEADS // KVH
C2 = HD ** (-0.5) * math.log2(math.e)
CAP = 2
CHUNK = 8
BF = jnp.bfloat16
F32 = jnp.float32


def params(mib=48, semantics=None):
    return pltpu.CompilerParams(
        vmem_limit_bytes=mib << 20, dimension_semantics=semantics
    )


def nt(a, b):
    return lax.dot_general(a, b, (((1,), (1,)), ((), ())), preferred_element_type=F32)


def mm(a, b):
    return jnp.dot(a, b, preferred_element_type=F32)


def hi_lo(x):
    hi = x.astype(BF)
    return hi, (x - hi.astype(F32)).astype(BF)


def scores(q, chunks, s_ref):
    top, at = None, 0
    for k, visible in chunks:
        s = nt(q, k) * C2
        if visible is not None:
            s = jnp.where(visible, s, -1e30)
        s_ref[:, at : at + k.shape[0]] = s
        m = jnp.max(s, axis=1, keepdims=True)
        top = m if top is None else jnp.maximum(top, m)
        at += k.shape[0]
    return top


def weigh(s_ref, values, top, state, span=512):
    if state is not None:
        before, lse = state
        top = jnp.maximum(top, lse)
    acc = None
    for at in range(0, s_ref.shape[1], span):
        cols = slice(at, min(at + span, s_ref.shape[1]))
        part = mm(jnp.exp2(s_ref[:, cols] - top).astype(BF), values[cols, :])
        acc = part if acc is None else acc + part
    out, total = acc[:, :HD], acc[:, HD : HD + 1]
    if state is not None:
        a = jnp.exp2(lse - top)
        out, total = out + before * a, total + a
    return out / total, top + jnp.log2(total)


def with_ones(ref, values):
    at = 0
    for v in values:
        ref[at : at + v.shape[0], :HD] = v
        ref[at : at + v.shape[0], HD:] = jnp.ones(v.shape, BF)
        at += v.shape[0]


def lane_of(stats, h):
    lane = lax.broadcasted_iota(jnp.int32, stats.shape, 1)
    return jnp.sum(jnp.where(lane == h, stats, 0.0), axis=1, keepdims=True)


def visible_rows(par_ref):
    n = par_ref.shape[0]
    rows = lax.broadcasted_iota(jnp.int32, (n, n), 0)
    cols = lax.broadcasted_iota(jnp.int32, (n, n), 1)
    side = n // 4
    block = side // 4
    starts = [z * side + x * block for x in range(4) for z in range(4)]
    parents = jnp.concatenate([par_ref[at : at + block, :] for at in starts], axis=0)
    number = cols // block % 4 * side + cols // side * block + cols % block
    step = ((parents == number).astype(F32) + (rows == cols).astype(F32)).astype(BF)
    two = mm(step, step).astype(BF)
    four = mm(two, two).astype(BF)
    six = mm(four, two).astype(BF)
    return mm(six, step) > 0.5


def heads_body(k_refs, v_refs, q_ref, before, o_ref, l_ref, v1, s0, s1):
    chunks = [(r[...], None) for r in k_refs]
    with_ones(v1, [r[...] for r in v_refs])

    def q_of(h):
        return q_ref[:, pl.ds(pl.multiple_of(h * HD, HD), HD)]

    def one(h, s_ref, top, stats):
        cols = pl.ds(pl.multiple_of(h * HD, HD), HD)
        state = None if before is None else (before[0][:, cols], lane_of(before[1][...], h))
        o, lse = weigh(s_ref, v1, top, state)
        o_ref[:, cols] = o
        lane = lax.broadcasted_iota(jnp.int32, stats.shape, 1)
        return jnp.where(lane == h, lse, stats)

    def pair(i, carry):
        top, stats = carry
        h = 2 * i
        after = scores(q_of(h + 1), chunks, s1)
        stats = one(h, s0, top, stats)
        top = scores(q_of(jnp.minimum(h + 2, GROUP - 1)), chunks, s0)
        return top, one(h + 1, s1, after, stats)

    first = scores(q_of(0), chunks, s0)
    l_ref[...] = lax.fori_loop(0, GROUP // 2, pair, (first, jnp.zeros(l_ref.shape, F32)), unroll=4)[1]


def state_shapes(rows):
    return [jax.ShapeDtypeStruct((rows, GROUP * HD), F32), jax.ShapeDtypeStruct((rows, HD), F32)]


def heads_scratch(rows, count):
    return [pltpu.VMEM((count, 2 * HD), BF), pltpu.VMEM((rows, count), F32), pltpu.VMEM((rows, count), F32)]


def start_body(idx, q_ref, k_ref, v_ref, o_ref, l_ref, *scratch):
    del idx
    heads_body([k_ref], [v_ref], q_ref, None, o_ref, l_ref, *scratch)


def attend_start(idx, q_all, keys, values):
    rows, count = q_all.shape[0], keys.shape[0]
    whole = lambda shape: pl.BlockSpec(shape, lambda i, idx: (0, 0))
    return pl.pallas_call(
        start_body,
        out_shape=state_shapes(rows),
        grid_spec=pltpu.PrefetchScalarGridSpec(
            num_scalar_prefetch=1,
            grid=(1,),
            in_specs=[
                whole(q_all.shape),
                pl.BlockSpec((count, HD), lambda i, idx: (0, idx[1])),
                pl.BlockSpec((count, HD), lambda i, idx: (0, idx[1])),
            ],
            out_specs=[whole(v.shape) for v in state_shapes(rows)],
            scratch_shapes=heads_scratch(rows, count),
        ),
        compiler_params=params(24),
        name="attend_start",
    )(idx, q_all, keys, values)


def more_body(q_ref, so_ref, sl_ref, b_ref, c_ref, o_ref, l_ref, *scratch):
    n = b_ref.shape[0] // 2
    keys, values = [[r.at[at] for r in (b_ref, c_ref)] for at in (pl.ds(0, n), pl.ds(n, n))]
    heads_body(keys, values, q_ref, (so_ref, sl_ref), o_ref, l_ref, *scratch)


def attend_more(q_all, state, parts):
    rows = q_all.shape[0]
    return pl.pallas_call(
        more_body,
        out_shape=state_shapes(rows),
        scratch_shapes=heads_scratch(rows, parts[0].shape[0]),
        compiler_params=params(24),
        name="attend_more",
    )(q_all, *state, *parts)


def last_body(shifts, idx, q_ref, so_ref, sl_ref, b_ref, *rest):
    n = b_ref.shape[0] // 2
    chunks, values = [(b_ref[:n, :], None)], [b_ref[n:, :]]
    if shifts == (0,):
        par_ref, sk_ref, sv_ref, *rest = rest
        chunks.append((sk_ref[...], visible_rows(par_ref)))
        values.append(sv_ref[...])
    outs, (v1, *held) = rest[: len(shifts)], rest[len(shifts) :]
    with_ones(v1, values)
    rows = q_ref.shape[0]
    lane = lax.broadcasted_iota(jnp.int32, (rows, HD), 1)
    heads = [(idx[0] + d) % (GROUP // 2) * 2 + h for d in shifts for h in range(2)]
    columns = [pl.ds(pl.multiple_of(h * HD, HD), HD) for h in heads]
    tops = {0: scores(q_ref[:, columns[0]], chunks, held[0])}
    for i, (head, cols) in enumerate(zip(heads, columns)):
        if i + 1 < len(heads):
            tops[i + 1] = scores(q_ref[:, columns[i + 1]], chunks, held[(i + 1) % len(held)])
        state = so_ref[:, cols], lane_of(sl_ref[...], head)
        o, lse = weigh(held[i % len(held)], v1, tops[i], state)
        h, o_ref = i % 2, outs[i // 2]
        stats = jnp.zeros((rows, HD), F32) if h == 0 else stats
        o_ref[:rows, h * HD : (h + 1) * HD] = o.astype(BF)
        left = lse
        for part in range(3):
            piece = left.astype(BF).astype(F32)
            left = left - piece
            stats = jnp.where(lane == 3 * h + part, piece, stats)
        if h == 1:
            o_ref[rows:, :] = stats.T[:16, :].astype(BF)


def attend_last(shifts, idx, q_all, state, part, extra):
    rows = q_all.shape[0]
    whole = lambda shape: pl.BlockSpec(shape, lambda i, idx: (0, 0))
    args = [q_all, *state, part]
    specs = [whole(v.shape) for v in args]
    count = part.shape[0] // 2
    if shifts == (0,):
        at = GROUP
        specs += [
            whole((rows, 1)),
            pl.BlockSpec((rows, HD), lambda i, idx: (0, at)),
            pl.BlockSpec((rows, HD), lambda i, idx: (0, at + 1)),
        ]
        args += [extra, q_all, q_all]
        count += rows
    shape = (rows + 16, 2 * HD)
    return pl.pallas_call(
        lambda *refs: last_body(shifts, *refs),
        out_shape=[jax.ShapeDtypeStruct(shape, BF)] * len(shifts),
        grid_spec=pltpu.PrefetchScalarGridSpec(
            num_scalar_prefetch=1,
            grid=(1,),
            in_specs=specs,
            out_specs=[whole(shape)] * len(shifts),
            scratch_shapes=[pltpu.VMEM((count, 2 * HD), BF), *[pltpu.VMEM((rows, count), F32)] * 2],
        ),
        compiler_params=params(24),
        name="attend_own" if shifts == (0,) else "attend_last",
    )(idx, *args)


def combine(parts, att):
    rows = att.shape[0]
    r = lax.broadcasted_iota(jnp.int32, (rows, rows), 0)
    c = lax.broadcasted_iota(jnp.int32, (rows, rows), 1)
    eye = (r == c).astype(F32).astype(BF)
    stats = [p[rows:, :].astype(F32) for p in parts]
    shares = []
    for h in range(2):
        at = 3 * h
        lse = [s[at : at + 1, :] + s[at + 1 : at + 2, :] + s[at + 2 : at + 3, :] for s in stats]
        top = jnp.maximum(jnp.maximum(lse[0], lse[1]), jnp.maximum(lse[2], lse[3]))
        w = [jnp.exp2(v - top) for v in lse]
        inv = 1.0 / (w[0] + w[1] + w[2] + w[3])
        shares += [v * inv for v in w]
    high, low = hi_lo(jnp.concatenate(shares + shares, axis=0))
    columns = nt(eye, high) + nt(eye, low)
    for h in range(2):
        cols = slice(h * HD, (h + 1) * HD)
        acc = sum(p[:rows, cols].astype(F32) * columns[:, 4 * h + i : 4 * h + i + 1] for i, p in enumerate(parts))
        att[:, cols] = acc.astype(BF)


def project_body(*refs):
    *parts, w_ref, o_ref, mixed_rows, att = refs

    @pl.when(pl.program_id(0) == 0)
    def _():
        combine(parts, mixed_rows)
        side = att.shape[0] // 4
        block = side // 4
        for z in range(4):
            for x in range(4):
                to, come = z * side + x * block, x * side + z * block
                att[to : to + block, :] = mixed_rows[come : come + block, :]

    o_ref[...] = mm(att[...], w_ref[...]).astype(BF)


def project(parts, weights, steps=4):
    rows, width = parts[0].shape[0] - 16, weights.shape[1]
    return pl.pallas_call(
        project_body,
        out_shape=pltpu.HBM((rows, width), BF),
        grid=(steps,),
        in_specs=[
            *[pl.BlockSpec(parts[0].shape, lambda i: (0, 0))] * 4,
            pl.BlockSpec((weights.shape[0], width // steps), lambda i: (0, i)),
        ],
        out_specs=pl.BlockSpec((rows, width // steps), lambda i: (0, i)),
        scratch_shapes=[pltpu.VMEM((rows, 2 * HD), BF), pltpu.VMEM((rows, 2 * HD), BF)],
        compiler_params=params(24),
        name="project",
    )(*parts, weights)


def route_body(p_ref, res_ref, gain_ref, router_ref, hot_ref, sel_ref, pack_ref, mixed_ref, gates_ref, buf, router_buf, sem):
    fetch = pltpu.make_async_copy(router_ref, router_buf, sem.at[4])
    fetch.start()
    rows, width = res_ref.shape
    step = width // CHUNK
    kept = []
    for c in range(CHUNK):
        cols = slice(c * step, (c + 1) * step)
        acc = res_ref[:, cols].astype(F32)
        for j in range(p_ref.shape[0] // rows):
            acc = acc + p_ref[j * rows : (j + 1) * rows, cols].astype(F32)
        mixed_ref[:, cols] = acc
        kept.append(acc)
    square = sum(jnp.sum(a * a, axis=1, keepdims=True) for a in kept)
    inverse = lax.rsqrt(square / width + EPSILON)
    normed = [(a * inverse * gain_ref[:, c * step : (c + 1) * step]).astype(BF) for c, a in enumerate(kept)]
    rows = jnp.concatenate(normed, axis=0)
    pieces = pack_ref.shape[0] // 4
    copies = []
    for j in range(4):
        at = pl.ds(j * pieces, pieces)
        buf[at, :] = mm(sel_ref[at, :], rows).astype(BF)
        copies.append(pltpu.make_async_copy(buf.at[at], pack_ref.at[at], sem.at[j]))
        copies[-1].start()
    fetch.wait()
    logits = sum(mm(n, router_buf[c * step : (c + 1) * step, :]) for c, n in enumerate(normed))
    sig = hot_ref[...] * jax.nn.sigmoid(logits)
    gates_ref[...] = sig / jnp.sum(sig, axis=1, keepdims=True)
    for copy in copies:
        copy.wait()


def route(partial, residual, gain, router, hot, select):
    rows, width = residual.shape
    step = width // CHUNK
    experts = router.shape[1]
    whole = lambda shape: pl.BlockSpec(shape, lambda i: (0, 0))
    router = pltpu.with_memory_space_constraint(router, pltpu.HBM)
    args = (partial, residual, gain, router, hot, select)
    return pl.pallas_call(
        route_body,
        out_shape=(
            pltpu.HBM((select.shape[0], step), BF),
            jax.ShapeDtypeStruct((rows, width), F32),
            jax.ShapeDtypeStruct((rows, experts), F32),
        ),
        grid=(1,),
        in_specs=[pl.BlockSpec(memory_space=pltpu.HBM) if v is router else whole(v.shape) for v in args],
        out_specs=(
            pl.BlockSpec(memory_space=pltpu.HBM),
            whole((rows, width)),
            whole((rows, experts)),
        ),
        scratch_shapes=[
            pltpu.VMEM((select.shape[0], step), BF),
            pltpu.VMEM(router.shape, BF),
            pltpu.SemaphoreType.DMA((5,)),
        ],
        compiler_params=params(),
        name="route",
    )(*args)


def shuffle_matrix():
    n = 16 * CAP * CHUNK
    to = lax.broadcasted_iota(jnp.int32, (n, n), 0)
    come = lax.broadcasted_iota(jnp.int32, (n, n), 1)
    tokens = 16 * CAP
    chunk = come % CHUNK
    token = come // CHUNK
    return (to == chunk * tokens + token).astype(F32).astype(BF)


STEPS = 4


def expert_body(perm_ref, back_ref, x_in, g_hbm, u_hbm, d_hbm, o_hbm, x, g, u, d, act, y, out, sems, out_sems):
    block = perm_ref.shape[0]
    tokens = block // CHUNK
    depth = g.shape[1]
    span = d.shape[2]
    count = x_in.shape[0] // block
    fetch = []
    for k in range(STEPS):
        for j, (src, dst) in enumerate(((g_hbm, g), (u_hbm, u))):
            at = pl.ds(k * depth, depth)
            fetch.append(pltpu.make_async_copy(src.at[at, :], dst.at[k], sems.at[2 * k + j]))
    for k in range(STEPS):
        at = pl.ds(k * span, span)
        fetch.append(pltpu.make_async_copy(d_hbm.at[:, at], d.at[k], sems.at[2 * STEPS + k]))
    for copy in fetch:
        copy.start()
    step = x_in.shape[1]
    for b in range(count):
        z = mm(perm_ref[...], x_in[b * block : (b + 1) * block, :]).astype(BF)
        for c in range(CHUNK):
            x[b * tokens : (b + 1) * tokens, c * step : (c + 1) * step] = z[c * tokens : (c + 1) * tokens, :]
    gate = up = None
    for k in range(STEPS):
        piece = x[:, k * depth : (k + 1) * depth]
        fetch[2 * k].wait()
        part = mm(piece, g[k])
        gate = part if gate is None else gate + part
        fetch[2 * k + 1].wait()
        part = mm(piece, u[k])
        up = part if up is None else up + part
    act[...] = (jax.nn.silu(gate) * up).astype(BF)
    for k in range(STEPS):
        fetch[2 * STEPS + k].wait()
        y[:, k * span : (k + 1) * span] = mm(act[...], d[k]).astype(BF)
    sends = []
    for b in range(count):
        rows = slice(b * tokens, (b + 1) * tokens)
        z = jnp.concatenate([y[rows, c * step : (c + 1) * step] for c in range(CHUNK)], axis=0)
        at = pl.ds(b * block, block)
        out[at, :] = mm(back_ref[...], z).astype(BF)
        sends.append(pltpu.make_async_copy(out.at[at], o_hbm.at[at], out_sems.at[b]))
        sends[-1].start()
    for copy in sends:
        copy.wait()


def expert(arrived, perm, back, gate_w, up_w, down_w):
    width, hidden = gate_w.shape
    total, step = arrived.shape
    tokens = total // CHUNK
    blocks = total // perm.shape[0]
    whole = lambda shape: pl.BlockSpec(shape, lambda i: (0, 0))
    hbm = pl.BlockSpec(memory_space=pltpu.HBM)
    return pl.pallas_call(
        expert_body,
        out_shape=pltpu.HBM(arrived.shape, BF),
        grid=(1,),
        in_specs=[whole(perm.shape), whole(back.shape), whole(arrived.shape), hbm, hbm, hbm],
        out_specs=hbm,
        scratch_shapes=[
            pltpu.VMEM((tokens, width), BF),
            pltpu.VMEM((STEPS, width // STEPS, hidden), BF),
            pltpu.VMEM((STEPS, width // STEPS, hidden), BF),
            pltpu.VMEM((STEPS, hidden, width // STEPS), BF),
            pltpu.VMEM((tokens, hidden), BF),
            pltpu.VMEM((tokens, width), BF),
            pltpu.VMEM((total, step), BF),
            pltpu.SemaphoreType.DMA((3 * STEPS,)),
            pltpu.SemaphoreType.DMA((blocks,)),
        ],
        compiler_params=params(),
        name="expert",
    )(perm, back, arrived, gate_w, up_w, down_w)


def finish_body(ret_ref, mask_ref, gates_ref, mixed_ref, o_ref):
    rows, experts = gates_ref.shape
    span = ret_ref.shape[0]
    step = ret_ref.shape[1]
    e = lax.broadcasted_iota(jnp.int32, (experts, span), 0)
    at = lax.broadcasted_iota(jnp.int32, (experts, span), 1)
    spread = (e == at // (span // experts)).astype(F32).astype(BF)
    high, low = hi_lo(gates_ref[...])
    wide = mm(high, spread) + mm(low, spread)
    weights = jnp.concatenate([wide] * CHUNK, axis=0) * mask_ref[...].astype(F32)
    high, low = hi_lo(weights)
    moe = mm(high, ret_ref[...]) + mm(low, ret_ref[...])
    for c in range(CHUNK):
        cols = slice(c * step, (c + 1) * step)
        o_ref[:, cols] = (mixed_ref[:, cols] + moe[c * rows : (c + 1) * rows, :]).astype(BF)


def finish(returned, mask, gates, mixed):
    return pl.pallas_call(
        finish_body,
        out_shape=jax.ShapeDtypeStruct(mixed.shape, BF),
        compiler_params=params(),
        name="finish",
    )(returned, mask, gates, mixed)


SHIFTS = (1, 3, 2)


def ready_body(idx, q_hbm, k_hbm, v_hbm, keys_hbm, values_hbm, o_ref, *rest):
    *pieces, q_ref, k_ref, v_ref, sems = rest
    fetch = [
        pltpu.make_async_copy(src, dst, sems.at[i])
        for i, (src, dst) in enumerate(((q_hbm, q_ref), (k_hbm, k_ref), (v_hbm, v_ref)))
    ]
    count = keys_hbm.shape[0]
    send = []
    for d, piece in zip(SHIFTS, pieces):
        cols = pl.ds(pl.multiple_of((idx[1] + d) % KVH * HD, HD), HD)
        for j, src in enumerate((keys_hbm, values_hbm)):
            to = piece.at[pl.ds(j * count, count), :]
            send.append(pltpu.make_async_copy(src.at[:, cols], to, sems.at[len(fetch) + len(send)]))
    for copy in fetch + send:
        copy.start()
    for copy in fetch:
        copy.wait()
    rows, wide = q_ref.shape[0], q_ref.shape[1] // KVH
    for z in range(KVH):
        at = slice(z * rows, (z + 1) * rows)
        o_ref[at, :wide] = q_ref[:, z * wide : (z + 1) * wide]
        o_ref[at, wide : wide + HD] = k_ref[:, z * HD : (z + 1) * HD]
        o_ref[at, wide + HD :] = v_ref[:, z * HD : (z + 1) * HD]
    for copy in send:
        copy.wait()


def ready(idx, *arrays):
    rows, count = arrays[0].shape[0], arrays[3].shape[0]
    arrays = [pltpu.with_memory_space_constraint(a, pltpu.HBM) for a in arrays]
    shape = (KVH * rows, (GROUP + 2) * HD)
    hbm = pl.BlockSpec(memory_space=pltpu.HBM)
    return pl.pallas_call(
        ready_body,
        out_shape=[pltpu.HBM(shape, BF), *[pltpu.HBM((2 * count, HD), BF)] * len(SHIFTS)],
        grid_spec=pltpu.PrefetchScalarGridSpec(
            num_scalar_prefetch=1,
            grid=(1,),
            in_specs=[hbm] * len(arrays),
            out_specs=[
                pl.BlockSpec(shape, lambda i, idx: (0, 0)),
                *[pl.BlockSpec((2 * count, HD), lambda i, idx: (0, 0))] * len(SHIFTS),
            ],
            scratch_shapes=[
                *[pltpu.VMEM(a.shape, BF) for a in arrays[:3]],
                pltpu.SemaphoreType.DMA((3 + 2 * len(SHIFTS),)),
            ],
        ),
        compiler_params=params(24),
        name="ready",
    )(idx, *arrays)


def local(
    queries,
    prefix_keys,
    prefix_values,
    suffix_keys,
    suffix_values,
    parents,
    out_proj,
    residual,
    norm_gain,
    router,
    routes,
    expert_gate,
    expert_up,
    expert_down,
):
    seq_count = lax.axis_size("seq")
    side = KVH
    across = seq_count // side
    s = lax.axis_index("seq")
    z, x = s // across, s % across
    q, sk, sv = queries[0], suffix_keys[0], suffix_values[0]
    rows = q.shape[0]
    keys, values = prefix_keys[0], prefix_values[0]
    place = jnp.stack([x, z]).astype(jnp.int32)
    copies, *pieces = ready(place, q, sk, sv, keys, values)
    parts = []
    for d, piece in zip(SHIFTS, pieces):
        parts.append(lax.ppermute(piece, "seq", [(i, (i + d * across) % seq_count) for i in range(seq_count)]))
    columns = [[i * across + j for i in range(side)] for j in range(across)]
    lines = [[i * across + j for j in range(across)] for i in range(side)]
    mine = lax.all_to_all(
        copies.reshape(side, rows, -1), "seq", 0, 0, tiled=True, axis_index_groups=columns
    ).reshape(copies.shape)
    q_all = lax.all_to_all(
        jnp.broadcast_to(mine, (across, *mine.shape)), "seq", 0, 0, tiled=True, axis_index_groups=lines
    )
    q_all = q_all.reshape(across * mine.shape[0], -1)
    state = attend_start(place, q_all, keys, values)
    state = attend_more(q_all, state, parts[:2])
    along_x = lambda a, d: lax.ppermute(
        a, "seq", [(i, i // across * across + (i + d) % across) for i in range(seq_count)]
    )
    others = (2, 1, 3)
    blocks = attend_last(others, place, q_all, state, parts[2], None)
    blocks = [along_x(block, d) for d, block in zip(others, blocks)]
    blocks += attend_last((0,), place, q_all, state, parts[2], parents[0][:, None])
    projected = project(blocks, out_proj)
    arrived = lax.all_to_all(
        projected.reshape(seq_count, rows, -1), "seq", 0, 0, tiled=True
    ).reshape(projected.shape)
    experts = router.shape[1]
    ids = routes[0]
    hot = jnp.any(ids[:, :, None] == jnp.arange(experts, dtype=jnp.int32), axis=1)
    before = jnp.cumsum(hot.astype(jnp.int32), axis=0) - hot
    slots = hot[:, :, None] & (before[:, :, None] == jnp.arange(CAP, dtype=jnp.int32))
    same = jnp.eye(CHUNK, dtype=jnp.bool_)
    mask = slots[None, :, :, :, None] & same[:, None, None, None, :]
    mask = mask.reshape(CHUNK * rows, experts * CAP * CHUNK).astype(BF)
    chosen = jnp.moveaxis(slots, 0, 2)
    select = chosen[:, :, None, None, :] & same[None, None, :, :, None]
    select = select.reshape(experts * CAP * CHUNK, CHUNK * rows).astype(BF)
    packed, mixed, gates = route(arrived, residual[0], norm_gain[None, :], router, hot.astype(F32), select)
    exchange = lambda a: lax.all_to_all(
        a.reshape(experts, CAP * CHUNK, -1), ("seq", "grp"), 0, 0, tiled=True
    ).reshape(a.shape)
    order = shuffle_matrix()
    finished = expert(exchange(packed), order, order.T, expert_gate[0], expert_up[0], expert_down[0])
    return finish(exchange(finished), mask, gates, mixed)[None]


def solution(mesh):
    rows = P("grp", "seq", None)
    spread = P(("seq", "grp"), None, None)
    in_specs = (
        rows, rows, rows, rows, rows, P("grp", None), P("seq", None), rows, P(), P(), rows, spread, spread, spread,
    )

    return jax.shard_map(local, mesh=mesh, in_specs=in_specs, out_specs=rows, check_vma=False)
```
